32 devices in a mesh: layer: 4 (over x, core), harm: 8 (over z, y).
Axes of the slice: x: 2, y: 2, z: 4, core: 2. Of those that a mesh axis runs over, the one named last changes fastest.
Arguments:
- source: bfloat16 [2, 2048, 128], P(None, 'harm'), may hold values from -6 to 6
- transfer: bfloat16 [4, 2, 2048, 2048], P('layer', None, 'harm'), may hold values from -0.09375 to 0.09375
- fields: bfloat16 [4, 2, 2048, 128], P('layer', None, 'harm'), may hold values from -6 to 6
- orders: int32 [2048], replicated, may hold values from 0 to 2047, each once
Outputs:
- gradients: float32 [4, 2, 4096], P('layer', None, 'harm')
- boundary: bfloat16 [4, 2, 2048, 128], P('layer', None, 'harm')
The draws below stay inside these ranges and needn't reach their ends.
Inputs may be any that keep to these rules, and one draw needn't show every extreme that they name: `orders`: every value from 0 to 2047 appears exactly once.
All inputs are finite; a program needn't handle non-finite values.
Results may differ from the reference program's by a relative error of at most 0.006.
Values may be sent and summed in bfloat16 or wider, within the bound.
No kernel may reach another device: no remote copies, remote signals or barrier semaphores. Data moves between devices by JAX's collectives and lax.ppermute only.
A program may use at most 64 MiB of HBM per device.

```python
import math
import jax
import jax.numpy as jnp
from jax import lax

HARM = 2048
LAYERS_DEV = 1
BATCH = 128
LAYERS = 4
N_HARM = 8


def shard_levels(key, extent, shards, least, high):
    def one(dim, blocks):
        draws = jax.random.uniform(jax.random.fold_in(jax.random.fold_in(key, 6), dim), (blocks,), jnp.float32, least / len(shards), high / len(shards))
        return jnp.repeat(jnp.exp(draws), extent[dim] // blocks).reshape((-1,) + (1,) * (len(extent) - dim - 1))

    level = one(*shards[0])
    for cut in shards[1:]:
        level = level * one(*cut)
    return level


def normal_values(stream_key, shape, deviation, bound, cuts=(), kind=jnp.bfloat16):
    drawn = jax.random.normal(stream_key, shape, jnp.float32) * deviation
    if len(cuts) > 0:
        drawn = shard_levels(stream_key, shape, cuts, -0.22, 0.18) * drawn
    return jnp.clip(drawn, min=-bound, max=bound).astype(kind)


def setup_inputs(seed: int = 0) -> dict:
    splits = jax.random.split(jax.random.key(seed), 5)
    source = normal_values(splits[0], (2, HARM, BATCH), 1.0, 6.0, ((1, 8),))
    transfer = normal_values(splits[1], (LAYERS, 2, HARM, HARM), (2 * HARM) ** -0.5, 0.09375, ((0, 4), (2, 8)))
    fields = normal_values(splits[2], (LAYERS, 2, HARM, BATCH), 1.0, 6.0, ((0, 4), (2, 8)))
    orders = jax.random.permutation(splits[3], HARM).astype(jnp.int32)
    return dict(source=source, transfer=transfer, fields=fields, orders=orders)


def correlate(adjoint, forward, position, band_start, band_width):
    harmonics = adjoint.shape[1]
    columns = adjoint.shape[2]
    adj_sorted = jnp.take(adjoint, position, axis=1).astype(jnp.float32)
    fwd_sorted = jnp.take(forward, position, axis=1).astype(jnp.float32)
    padded = jnp.pad(adj_sorted, ((0, 0), (harmonics, harmonics + 1), (0, 0)))
    window_slab = lax.dynamic_slice_in_dim(padded, band_start + 1, harmonics + band_width, 1)
    count = harmonics // band_width
    blocks = window_slab.reshape(2, count + 1, band_width, columns)
    windows = jnp.concatenate([blocks[:, :-1], blocks[:, 1:]], axis=2)
    forward_blocks = fwd_sorted.reshape(2, count, band_width, columns)

    def product(left_part, right_part):
        return jnp.einsum('nkb,ncb->nkc', left_part, right_part)
    real_part = product(forward_blocks[0], windows[0]) - product(forward_blocks[1], windows[1])
    imag_part = product(forward_blocks[0], windows[1]) + product(forward_blocks[1], windows[0])

    def diagonals(result_block):
        flattened = result_block.reshape(count, band_width * 2 * band_width)
        flattened = jnp.pad(flattened, ((0, 0), (0, band_width)))
        shaped = flattened.reshape(count, band_width, 2 * band_width + 1)[:, :, :band_width]
        return lax.optimization_barrier(jnp.sum(shaped, axis=(0, 1)))
    return jnp.stack([diagonals(real_part), diagonals(imag_part)])

def reference(source, transfer, fields, orders):
    harmonics = orders.shape[0]
    columns = source.shape[2]
    layer_count = transfer.shape[0]
    position = jnp.zeros((harmonics,), jnp.int32).at[orders].set(jnp.arange(harmonics, dtype=jnp.int32))
    band_width = 2 * harmonics // N_HARM
    norm_scale = 1.0 / math.sqrt(harmonics * columns)
    starts = jnp.arange(0, 2 * harmonics, band_width, dtype=jnp.int32)
    adjoint = source
    grads = [None] * layer_count
    bounds = []
    for layer_index in range(layer_count - 1, -1, -1):
        forward = fields[layer_index]
        bands = lax.map(lambda band_start: correlate(adjoint, forward, position, band_start, band_width), starts)
        grads[layer_index] = jnp.transpose(bands, (1, 0, 2)).reshape(2, 2 * harmonics) * norm_scale
        matrix = transfer[layer_index]
        real_part = jnp.dot(matrix[0], adjoint[0], preferred_element_type=jnp.float32) - jnp.dot(matrix[1], adjoint[1], preferred_element_type=jnp.float32)
        imag_part = jnp.dot(matrix[0], adjoint[1], preferred_element_type=jnp.float32) + jnp.dot(matrix[1], adjoint[0], preferred_element_type=jnp.float32)
        adjoint = jnp.stack([real_part, imag_part]).astype(jnp.bfloat16)
        if layer_index % LAYERS_DEV == 0:
            bounds.append(adjoint)
    return (jnp.stack(grads), jnp.stack(bounds[::-1]))
```

```python
import math

import jax
import jax.numpy as jnp
from jax import lax
from jax.experimental import pallas as pl
from jax.experimental.pallas import tpu as pltpu
from jax.sharding import PartitionSpec as P


LANES = 128
VMEM = pltpu.VMEM
BF16 = jnp.bfloat16
F32 = jnp.float32


def call(body, outs, args, limit, scratch=(), name=None):
    spec = pl.BlockSpec(memory_space=VMEM)
    return pl.pallas_call(
        body,
        out_shape=outs,
        in_specs=[spec] * len(args),
        out_specs=jax.tree.map(lambda _: spec, outs),
        scratch_shapes=list(scratch),
        compiler_params=pltpu.CompilerParams(vmem_limit_bytes=limit << 20),
        name=name,
    )(*[pltpu.with_memory_space_constraint(a, VMEM) for a in args])


def joined(value):
    return jnp.concatenate([value[0], value[1]], axis=1)


def partner(step, fan):
    return lax.axis_index("harm") ^ step if fan else 0


def product(matrix_ref, shards, fan):
    rows = matrix_ref.shape[1]
    part = jnp.zeros((rows, 2 * LANES), F32)
    by_re, by_im = part, part
    for step, value in enumerate(shards):
        size = value.shape[1]
        start = pl.multiple_of(partner(step, fan) * size, size) if fan else 0
        cols = pl.ds(start, size)
        both = joined(value)
        by_re += jnp.dot(matrix_ref[0, :, cols], both, preferred_element_type=F32)
        by_im += jnp.dot(matrix_ref[1, :, cols], both, preferred_element_type=F32)
    re = by_re[:, :LANES] - by_im[:, LANES:]
    im = by_re[:, LANES:] + by_im[:, :LANES]
    return re.astype(BF16), im.astype(BF16)


def propagate(matrix, shards, fan):
    def body(matrix_ref, *refs):
        out_ref = refs[-1]
        re, im = product(matrix_ref, [r[...] for r in refs[:-1]], fan)
        out_ref[0] = re
        out_ref[1] = im

    rows = matrix.shape[1]
    return call(body, VMEM((2, rows, LANES), BF16), [matrix, *shards], 8, name="propagate")


def one_hot(targets, first, count):
    index = lax.broadcasted_iota(jnp.int32, (count, targets.shape[1]), 0) + first
    return jnp.where(index == targets, 1.0, 0.0).astype(BF16)


def sort_fields(orders, shards, fan):
    harmonics = orders.shape[1]
    blocks = harmonics // LANES

    def body(orders_ref, *refs):
        shard_refs, out_ref, whole = refs[:-2], refs[-2], refs[-1]
        fill(whole, [r[...] for r in shard_refs], fan)
        targets = orders_ref[...] ^ (LANES - 1)
        chunk = 4 * LANES

        def step(c, carry):
            picked = jnp.dot(
                one_hot(targets, c * chunk, chunk), whole[...], preferred_element_type=F32
            ).astype(BF16)
            for b in range(chunk // LANES):
                re = picked[b * LANES : (b + 1) * LANES, :LANES]
                im = picked[b * LANES : (b + 1) * LANES, LANES:]
                at = pl.multiple_of((c * (chunk // LANES) + b) * 2 * LANES, LANES)
                out_ref[:LANES, pl.ds(at, LANES)] = re
                out_ref[:LANES, pl.ds(at + LANES, LANES)] = -im
                out_ref[LANES:, pl.ds(at, LANES)] = im
                out_ref[LANES:, pl.ds(at + LANES, LANES)] = re
            return carry

        lax.fori_loop(0, harmonics // chunk, step, 0)

    return call(
        body,
        VMEM((2 * LANES, blocks * 2 * LANES), BF16),
        [orders, *shards],
        24,
        [VMEM((harmonics, 2 * LANES), BF16)],
        name="sort_fields",
    )


def fill(whole, shards, fan):
    for step, value in enumerate(shards):
        size = value.shape[1]
        start = pl.multiple_of(partner(step, fan) * size, size) if fan else 0
        whole[pl.ds(start, size), :LANES] = value[0]
        whole[pl.ds(start, size), LANES:] = value[1]


def finish(matrix, orders, factors, sets, belows, fan, band, scale):
    layers = len(sets)
    harmonics = orders.shape[1]
    rows = matrix.shape[1]
    blocks = harmonics // LANES
    bands = band // LANES
    strip = bands + 1
    per_set = [len(s) for s in sets]

    def body(matrix_ref, orders_ref, factors_ref, *refs):
        refs = list(refs)
        set_refs = []
        for count in per_set:
            set_refs.append(refs[:count])
            refs = refs[count:]
        below_refs, refs = refs[: layers - 1], refs[layers - 1 :]
        grad_ref, bottom_ref, whole, moved = refs
        layer = lax.axis_index("layer")
        last = [r[...] for r in set_refs[0]]
        chosen = last
        for index in range(1, layers):
            chosen = [
                jnp.where(layer == index, r[...], c) for r, c in zip(set_refs[index], chosen)
            ]
        fill(whole, chosen, fan)
        re, im = product(matrix_ref, last, fan)
        for index in range(1, layers):
            re = jnp.where(layer == index, below_refs[index - 1][0], re)
            im = jnp.where(layer == index, below_refs[index - 1][1], im)
        bottom_ref[0, 0] = re
        bottom_ref[0, 1] = im

        targets = orders_ref[...] + (harmonics - 1 - band * lax.axis_index("harm"))
        for c in range(blocks + bands):
            picked = jnp.dot(
                one_hot(targets, c * LANES, LANES), whole[...], preferred_element_type=F32
            ).astype(BF16)
            moved[:, c * 2 * LANES : (c + 1) * 2 * LANES] = picked
        width = 2 * LANES
        length = blocks * width
        parts = []
        for q in range(strip):
            parts.append(
                lax.dot_general(
                    factors_ref[...],
                    moved[:, q * width : q * width + length],
                    (((1,), (1,)), ((), ())),
                    preferred_element_type=F32,
                )
            )
        strips = jnp.concatenate(parts, axis=1)
        size = strip * LANES
        for part in range(2):
            skewed = pltpu.roll(
                strips[part * LANES : (part + 1) * LANES],
                size - (LANES - 1),
                1,
                stride=1,
                stride_axis=0,
            )
            total = jnp.sum(skewed[:, :band], axis=0, keepdims=True) * scale
            grad_ref[0, pl.ds(part, 1), :] = total

    outs = (
        jax.ShapeDtypeStruct((1, 2, band), F32),
        jax.ShapeDtypeStruct((1, 2, rows, LANES), BF16),
    )
    args = [matrix, orders, factors]
    for group in sets:
        args += group
    args += belows
    return call(
        body,
        outs,
        args,
        24,
        [
            VMEM((harmonics, 2 * LANES), BF16),
            VMEM((LANES, (blocks + bands) * 2 * LANES), BF16),
        ],
        name="finish",
    )


def sweep(source, transfer, fields, orders):
    layers = lax.axis_size("layer")
    count = lax.axis_size("harm")
    harmonics = orders.shape[0]
    columns = source.shape[2]
    rows = source.shape[1]
    fan = rows % LANES == 0 and count & (count - 1) == 0
    band = 2 * harmonics // count
    scale = 1.0 / math.sqrt(harmonics * columns)
    axes = ("layer", "harm")
    matrix = transfer[0]
    table = orders.reshape(1, harmonics)
    steps = sorted(range(count), reverse=True)

    def to_layer(value, pick, target):
        if not fan:
            moved = value
            if pick(0) != target:
                pairs = [(pick(0) * count + h, target * count + h) for h in range(count)]
                moved = lax.ppermute(value, axes, pairs)
            return [lax.all_gather(moved, "harm", axis=1, tiled=True)]
        out = [None] * count
        for step in steps:
            origin = pick(step)
            if origin == target and step == 0:
                out[0] = value
                continue
            pairs = [(origin * count + h, target * count + (h ^ step)) for h in range(count)]
            out[step] = lax.ppermute(value, axes, pairs)
        return out

    def in_layer(value):
        if not fan:
            return [lax.all_gather(value, "harm", axis=1, tiled=True)]
        out = [value]
        for step in range(1, count):
            pairs = [
                (r * count + h, r * count + (h ^ step))
                for r in range(layers)
                for h in range(count)
            ]
            out.append(lax.ppermute(value, axes, pairs))
        return out

    top = layers - 1

    def replica(step):
        if not fan or step == 0 or layers == 1:
            return top
        return step % (layers - 1)

    shards = to_layer(source, replica, top)
    sets = [shards]
    belows = []
    factors = None
    for layer in range(top, 0, -1):
        below = propagate(matrix, shards, fan)
        belows.append(below)
        shards = to_layer(below, lambda step, layer=layer: layer, layer - 1)
        sets.append(shards)
        if layer == min(2, top):
            held, _ = lax.optimization_barrier((fields[0], below))
            mine = in_layer(held)
    if factors is None:
        factors = sort_fields(table, mine, fan)
    grads, bottom = finish(
        matrix, table, factors, sets[::-1], belows[::-1], fan, band, scale
    )
    return grads, bottom


def solution(mesh):
    return jax.shard_map(
        sweep,
        mesh=mesh,
        in_specs=(
            P(None, "harm", None),
            P("layer", None, "harm", None),
            P("layer", None, "harm", None),
            P(),
        ),
        out_specs=(P("layer", None, "harm"), P("layer", None, "harm", None)),
        check_vma=False,
    )
```

```python
import math

import jax
import jax.numpy as jnp
from jax import lax
from jax.experimental import pallas as pl
from jax.experimental.pallas import tpu as pltpu
from jax.sharding import PartitionSpec as P


LANES = 128
VMEM = pltpu.VMEM
BF16 = jnp.bfloat16
F32 = jnp.float32


def call(body, outs, args, limit, scratch=()):
    spec = pl.BlockSpec(memory_space=VMEM)
    return pl.pallas_call(
        body,
        out_shape=outs,
        in_specs=[spec] * len(args),
        out_specs=jax.tree.map(lambda _: spec, outs),
        scratch_shapes=list(scratch),
        compiler_params=pltpu.CompilerParams(vmem_limit_bytes=limit << 20),
    )(*[pltpu.with_memory_space_constraint(a, VMEM) for a in args])


def joined(value):
    return jnp.concatenate([value[0], value[1]], axis=1)


QUARTERS = {
    "far": (3, 2, 1, 0),
    "out": (1, 3, 0, 2),
    "in": (2, 0, 3, 1),
    "own": (0, 1, 2, 3),
}
ORDER = ("far0", "own1", "far1", "out0", "out1", "in0", "in1", "own0")


def routes(count):
    if count == len(ORDER):
        return [
            [QUARTERS[slot[:-1]][h // 2] * 2 + (h % 2 ^ int(slot[-1])) for h in range(count)]
            for slot in ORDER
        ]
    return [[(h + s) % count for h in range(count)] for s in range(count - 1, -1, -1)]


def partner(step, fan):
    if not fan:
        return 0
    targets = routes(lax.axis_size("harm"))[step]
    here = lax.axis_index("harm")
    origin = jnp.int32(targets.index(0))
    for spot in range(1, len(targets)):
        origin = jnp.where(here == spot, targets.index(spot), origin)
    return origin


def product(matrix_ref, shards, fan):
    rows = matrix_ref.shape[1]
    part = jnp.zeros((rows, 2 * LANES), F32)
    by_re, by_im = part, part
    for step, value in enumerate(shards):
        size = value.shape[1]
        start = pl.multiple_of(partner(step, fan) * size, size) if fan else 0
        cols = pl.ds(start, size)
        both = joined(value)
        by_re += jnp.dot(matrix_ref[0, :, cols], both, preferred_element_type=F32)
        by_im += jnp.dot(matrix_ref[1, :, cols], both, preferred_element_type=F32)
    re = by_re[:, :LANES] - by_im[:, LANES:]
    im = by_re[:, LANES:] + by_im[:, :LANES]
    return re.astype(BF16), im.astype(BF16)


def propagate(matrix, shards, fan):
    def body(matrix_ref, *refs):
        out_ref = refs[-1]
        re, im = product(matrix_ref, [r[...] for r in refs[:-1]], fan)
        out_ref[0] = re
        out_ref[1] = im

    rows = matrix.shape[1]
    return call(body, VMEM((2, rows, LANES), BF16), [matrix, *shards], 8)


def one_hot(targets, first, count):
    index = lax.broadcasted_iota(jnp.int32, (count, targets.shape[1]), 0) + first
    return jnp.where(index == targets, 1.0, 0.0).astype(BF16)


def bring(matrix, source, orders):
    args = [matrix, source, orders]

    def body(*refs):
        size = len(args)
        ins, outs, sems = refs[:size], refs[size : 2 * size], refs[-1]
        copies = [
            pltpu.make_async_copy(ins[i], outs[i], sems.at[i]) for i in range(size)
        ]
        for copy in copies:
            copy.start()
        for copy in copies:
            copy.wait()

    hbm = pl.BlockSpec(memory_space=pltpu.HBM)
    return pl.pallas_call(
        body,
        out_shape=[VMEM(a.shape, a.dtype) for a in args],
        in_specs=[hbm] * len(args),
        out_specs=[pl.BlockSpec(memory_space=VMEM)] * len(args),
        scratch_shapes=[pltpu.SemaphoreType.DMA((len(args),))],
        compiler_params=pltpu.CompilerParams(vmem_limit_bytes=1 << 20),
        name="bring",
    )(*[pltpu.with_memory_space_constraint(a, pltpu.HBM) for a in args])


def sort_fields(orders, groups, fan, split):
    harmonics = orders.shape[1]
    blocks = harmonics // LANES
    pieces = len(groups[0])

    def body(orders_ref, *refs):
        shard_refs, out_ref, whole = refs[:-2], refs[-2], refs[-1]
        values = [r[...] for r in shard_refs[:pieces]]
        if len(groups) > 1:
            low = lax.axis_index("layer") < split
            values = [
                jnp.where(low, v, r[...]) for v, r in zip(values, shard_refs[pieces:])
            ]
        fill(whole, values, fan)
        targets = orders_ref[...] ^ (LANES - 1)
        chunk = 4 * LANES

        def step(c, carry):
            picked = jnp.dot(
                one_hot(targets, c * chunk, chunk), whole[...], preferred_element_type=F32
            ).astype(BF16)
            for b in range(chunk // LANES):
                re = picked[b * LANES : (b + 1) * LANES, :LANES]
                im = picked[b * LANES : (b + 1) * LANES, LANES:]
                at = pl.multiple_of((c * (chunk // LANES) + b) * 2 * LANES, LANES)
                out_ref[:LANES, pl.ds(at, LANES)] = re
                out_ref[:LANES, pl.ds(at + LANES, LANES)] = -im
                out_ref[LANES:, pl.ds(at, LANES)] = im
                out_ref[LANES:, pl.ds(at + LANES, LANES)] = re
            return carry

        lax.fori_loop(0, harmonics // chunk, step, 0)

    return call(
        body,
        VMEM((2 * LANES, blocks * 2 * LANES), BF16),
        [orders, *[a for group in groups for a in group]],
        24,
        [VMEM((harmonics, 2 * LANES), BF16)],
    )


def fill(whole, shards, fan):
    for step, value in enumerate(shards):
        size = value.shape[1]
        start = pl.multiple_of(partner(step, fan) * size, size) if fan else 0
        whole[pl.ds(start, size), :LANES] = value[0]
        whole[pl.ds(start, size), LANES:] = value[1]


def finish(matrix, orders, factors, sets, belows, fan, band, scale):
    layers = len(sets)
    harmonics = orders.shape[1]
    rows = matrix.shape[1]
    blocks = harmonics // LANES
    bands = band // LANES
    strip = bands + 1
    per_set = [len(s) for s in sets]

    def body(matrix_ref, orders_ref, factors_ref, *refs):
        refs = list(refs)
        set_refs = []
        for count in per_set:
            set_refs.append(refs[:count])
            refs = refs[count:]
        below_refs, refs = refs[: layers - 1], refs[layers - 1 :]
        grad_ref, bottom_ref, whole, moved = refs
        layer = lax.axis_index("layer")
        last = [r[...] for r in set_refs[0]]
        chosen = last
        for index in range(1, layers):
            chosen = [
                jnp.where(layer == index, r[...], c) for r, c in zip(set_refs[index], chosen)
            ]
        fill(whole, chosen, fan)
        re, im = product(matrix_ref, last, fan)
        for index in range(1, layers):
            re = jnp.where(layer == index, below_refs[index - 1][0], re)
            im = jnp.where(layer == index, below_refs[index - 1][1], im)
        bottom_ref[0, 0] = re
        bottom_ref[0, 1] = im

        targets = orders_ref[...] + (harmonics - 1 - band * lax.axis_index("harm"))
        for c in range(blocks + bands):
            picked = jnp.dot(
                one_hot(targets, c * LANES, LANES), whole[...], preferred_element_type=F32
            ).astype(BF16)
            moved[:, c * 2 * LANES : (c + 1) * 2 * LANES] = picked
        width = 2 * LANES
        length = blocks * width
        parts = []
        for q in range(strip):
            parts.append(
                lax.dot_general(
                    factors_ref[...],
                    moved[:, q * width : q * width + length],
                    (((1,), (1,)), ((), ())),
                    preferred_element_type=F32,
                )
            )
        strips = jnp.concatenate(parts, axis=1)
        size = strip * LANES
        for part in range(2):
            skewed = pltpu.roll(
                strips[part * LANES : (part + 1) * LANES],
                size - (LANES - 1),
                1,
                stride=1,
                stride_axis=0,
            )
            total = jnp.sum(skewed[:, :band], axis=0, keepdims=True) * scale
            grad_ref[0, pl.ds(part, 1), :] = total

    outs = (
        jax.ShapeDtypeStruct((1, 2, band), F32),
        jax.ShapeDtypeStruct((1, 2, rows, LANES), BF16),
    )
    args = [matrix, orders, factors]
    for group in sets:
        args += group
    args += belows
    return call(
        body,
        outs,
        args,
        24,
        [
            VMEM((harmonics, 2 * LANES), BF16),
            VMEM((LANES, (blocks + bands) * 2 * LANES), BF16),
        ],
    )


def sweep_layers(source, transfer, fields, orders):
    layers = lax.axis_size("layer")
    count = lax.axis_size("harm")
    harmonics = orders.shape[0]
    columns = source.shape[2]
    rows = source.shape[1]
    fan = rows % LANES == 0 and layers > 3
    band = 2 * harmonics // count
    scale = 1.0 / math.sqrt(harmonics * columns)
    axes = ("layer", "harm")
    top = layers - 1
    plan = routes(count) if fan else []
    still = list(range(count))

    def gathered(value):
        return [lax.all_gather(value, "harm", axis=1, tiled=True)]

    def to_layer(value, origins, target):
        if not fan:
            if origins[0] != target:
                pairs = [(origins[0] * count + h, target * count + h) for h in range(count)]
                value = lax.ppermute(value, axes, pairs)
            return gathered(value)
        out = []
        for origin, route in zip(origins, plan):
            if origin == target and route == still:
                out.append(value)
                continue
            pairs = [(origin * count + h, target * count + route[h]) for h in range(count)]
            out.append(lax.ppermute(value, axes, pairs))
        return out

    def in_layers(value, members):
        out = []
        for route in plan:
            if route == still:
                out.append(value)
                continue
            pairs = [(r * count + h, r * count + route[h]) for r in members for h in range(count)]
            out.append(lax.ppermute(value, axes, pairs))
        return out

    matrix, own, table = bring(transfer[0], source, orders.reshape(1, harmonics))
    if fan:
        origins = [(s + 1) % (layers - 1) for s in range(count - 1)] + [top]
    else:
        origins = [top]
    shards = to_layer(source, origins, top)
    if fan:
        shards[-1] = own
    sets = [shards]
    belows = []
    early = tuple(r for r in range(layers) if r < layers // 2)
    late = tuple(r for r in range(layers) if r >= layers // 2)
    mine = []
    for layer in range(top, 0, -1):
        below = propagate(matrix, shards, fan)
        belows.append(below)
        shards = to_layer(below, [layer] * count, layer - 1)
        sets.append(shards)
        if fan and layer > top - 2:
            held, _ = lax.optimization_barrier((fields[0], below))
            mine.append(in_layers(held, early if layer == top else late))
    if not fan:
        mine = [gathered(fields[0])]
    factors = sort_fields(table, mine, fan, len(early))
    grads, bottom = finish(
        matrix, table, factors, sets[::-1], belows[::-1], fan, band, scale
    )
    return grads, bottom


def solution(mesh):
    return jax.shard_map(
        sweep_layers,
        mesh=mesh,
        in_specs=(
            P(None, "harm", None),
            P("layer", None, "harm", None),
            P("layer", None, "harm", None),
            P(),
        ),
        out_specs=(P("layer", None, "harm"), P("layer", None, "harm", None)),
        check_vma=False,
    )
```

```python
import math

import jax
import jax.numpy as jnp
from jax import lax
from jax.experimental import pallas as pl
from jax.experimental.pallas import tpu as pltpu
from jax.sharding import PartitionSpec as P


LANES = 128
VMEM = pltpu.VMEM
BF16 = jnp.bfloat16
F32 = jnp.float32


def call(body, outs, args, limit, scratch=()):
    spec = pl.BlockSpec(memory_space=VMEM)
    return pl.pallas_call(
        body,
        out_shape=outs,
        in_specs=[spec] * len(args),
        out_specs=jax.tree.map(lambda _: spec, outs),
        scratch_shapes=list(scratch),
        compiler_params=pltpu.CompilerParams(vmem_limit_bytes=limit << 20),
    )(*[pltpu.with_memory_space_constraint(a, VMEM) for a in args])


def joined(value):
    return jnp.concatenate([value[0], value[1]], axis=1)


QUARTERS = {
    "far": (3, 2, 1, 0),
    "out": (1, 3, 0, 2),
    "in": (2, 0, 3, 1),
    "own": (0, 1, 2, 3),
}
FEED = ("far", "out", "in", "own")
ORDER = ("far0", "own1", "far1", "out0", "out1", "in0", "in1", "own0")


def routes(count):
    half = count // 4
    return [
        [QUARTERS[slot[:-1]][h // half] * half + (h % half ^ int(slot[-1])) for h in range(count)]
        for slot in ORDER
    ]


def partner(step, fan):
    if not fan:
        return 0
    targets = routes(lax.axis_size("harm"))[step]
    here = lax.axis_index("harm")
    origin = jnp.int32(targets.index(0))
    for spot in range(1, len(targets)):
        origin = jnp.where(here == spot, targets.index(spot), origin)
    return origin


def product(matrix_ref, shards, fan):
    rows = matrix_ref.shape[1]
    part = jnp.zeros((rows, 2 * LANES), F32)
    by_re, by_im = part, part
    for step, value in enumerate(shards):
        size = value.shape[1]
        start = pl.multiple_of(partner(step, fan) * size, size) if fan else 0
        cols = pl.ds(start, size)
        both = joined(value)
        by_re += jnp.dot(matrix_ref[0, :, cols], both, preferred_element_type=F32)
        by_im += jnp.dot(matrix_ref[1, :, cols], both, preferred_element_type=F32)
    re = by_re[:, :LANES] - by_im[:, LANES:]
    im = by_re[:, LANES:] + by_im[:, :LANES]
    return re.astype(BF16), im.astype(BF16)


def propagate(matrix, shards, fan):
    def body(matrix_ref, *refs):
        out_ref = refs[-1]
        re, im = product(matrix_ref, [r[...] for r in refs[:-1]], fan)
        out_ref[0] = re
        out_ref[1] = im

    rows = matrix.shape[1]
    return call(body, VMEM((2, rows, LANES), BF16), [matrix, *shards], 8)


def one_hot(targets, first, count):
    index = lax.broadcasted_iota(jnp.int32, (count, targets.shape[1]), 0) + first
    return jnp.where(index == targets, 1.0, 0.0).astype(BF16)


def bring(matrix, source, orders):
    args = [matrix, source, orders]

    def body(*refs):
        size = len(args)
        ins, outs, sems = refs[:size], refs[size : 2 * size], refs[-1]
        copies = [
            pltpu.make_async_copy(ins[i], outs[i], sems.at[i]) for i in range(size)
        ]
        for copy in copies:
            copy.start()
        for copy in copies:
            copy.wait()

    hbm = pl.BlockSpec(memory_space=pltpu.HBM)
    return pl.pallas_call(
        body,
        out_shape=[VMEM(a.shape, a.dtype) for a in args],
        in_specs=[hbm] * len(args),
        out_specs=[pl.BlockSpec(memory_space=VMEM)] * len(args),
        scratch_shapes=[pltpu.SemaphoreType.DMA((len(args),))],
        compiler_params=pltpu.CompilerParams(vmem_limit_bytes=1 << 20),
        name="bring",
    )(*[pltpu.with_memory_space_constraint(a, pltpu.HBM) for a in args])


def sort_fields(orders, shards, fan):
    harmonics = orders.shape[1]
    blocks = harmonics // LANES

    def body(orders_ref, *refs):
        shard_refs, out_ref, whole = refs[:-2], refs[-2], refs[-1]
        if fan:
            here = lax.axis_index("harm")
            for name, ref in zip(FEED, shard_refs):
                quarter = jnp.int32(QUARTERS[name].index(0))
                for spot in range(1, 4):
                    quarter = jnp.where(here // 2 == spot, QUARTERS[name].index(spot), quarter)
                size = ref.shape[2]
                for part in range(2):
                    start = (quarter * 2 + (here % 2 ^ part)) * size
                    put(whole, pl.multiple_of(start, size), ref[part])
        else:
            put(whole, 0, shard_refs[0][...])
        targets = orders_ref[...] ^ (LANES - 1)
        chunk = 4 * LANES

        def step(c, carry):
            picked = jnp.dot(
                one_hot(targets, c * chunk, chunk), whole[...], preferred_element_type=F32
            ).astype(BF16)
            for b in range(chunk // LANES):
                re = picked[b * LANES : (b + 1) * LANES, :LANES]
                im = picked[b * LANES : (b + 1) * LANES, LANES:]
                at = pl.multiple_of((c * (chunk // LANES) + b) * 2 * LANES, LANES)
                out_ref[:LANES, pl.ds(at, LANES)] = re
                out_ref[:LANES, pl.ds(at + LANES, LANES)] = -im
                out_ref[LANES:, pl.ds(at, LANES)] = im
                out_ref[LANES:, pl.ds(at + LANES, LANES)] = re
            return carry

        lax.fori_loop(0, harmonics // chunk, step, 0)

    return call(
        body,
        VMEM((2 * LANES, blocks * 2 * LANES), BF16),
        [orders, *shards],
        24,
        [VMEM((harmonics, 2 * LANES), BF16)],
    )


def put(whole, start, value):
    rows = pl.ds(start, value.shape[1])
    whole[rows, :LANES] = value[0]
    whole[rows, LANES:] = value[1]


def fill(whole, shards, fan):
    for step, value in enumerate(shards):
        size = value.shape[1]
        start = pl.multiple_of(partner(step, fan) * size, size) if fan else 0
        put(whole, start, value)


def finish(matrix, orders, factors, sets, belows, fan, band, scale):
    layers = len(sets)
    harmonics = orders.shape[1]
    rows = matrix.shape[1]
    blocks = harmonics // LANES
    bands = band // LANES
    strip = bands + 1
    per_set = [len(s) for s in sets]

    def body(matrix_ref, orders_ref, factors_ref, *refs):
        refs = list(refs)
        set_refs = []
        for count in per_set:
            set_refs.append(refs[:count])
            refs = refs[count:]
        below_refs, refs = refs[: layers - 1], refs[layers - 1 :]
        grad_ref, bottom_ref, whole, moved = refs
        layer = lax.axis_index("layer")
        last = [r[...] for r in set_refs[0]]
        chosen = last
        for index in range(1, layers):
            chosen = [
                jnp.where(layer == index, r[...], c) for r, c in zip(set_refs[index], chosen)
            ]
        fill(whole, chosen, fan)
        re, im = product(matrix_ref, last, fan)
        for index in range(1, layers):
            re = jnp.where(layer == index, below_refs[index - 1][0], re)
            im = jnp.where(layer == index, below_refs[index - 1][1], im)
        bottom_ref[0, 0] = re
        bottom_ref[0, 1] = im

        targets = orders_ref[...] + (harmonics - 1 - band * lax.axis_index("harm"))
        for c in range(blocks + bands):
            picked = jnp.dot(
                one_hot(targets, c * LANES, LANES), whole[...], preferred_element_type=F32
            ).astype(BF16)
            moved[:, c * 2 * LANES : (c + 1) * 2 * LANES] = picked
        width = 2 * LANES
        length = blocks * width
        parts = []
        for q in range(strip):
            parts.append(
                lax.dot_general(
                    factors_ref[...],
                    moved[:, q * width : q * width + length],
                    (((1,), (1,)), ((), ())),
                    preferred_element_type=F32,
                )
            )
        strips = jnp.concatenate(parts, axis=1)
        size = strip * LANES
        for part in range(2):
            skewed = pltpu.roll(
                strips[part * LANES : (part + 1) * LANES],
                size - (LANES - 1),
                1,
                stride=1,
                stride_axis=0,
            )
            total = jnp.sum(skewed[:, :band], axis=0, keepdims=True) * scale
            grad_ref[0, pl.ds(part, 1), :] = total

    outs = (
        jax.ShapeDtypeStruct((1, 2, band), F32),
        jax.ShapeDtypeStruct((1, 2, rows, LANES), BF16),
    )
    args = [matrix, orders, factors]
    for group in sets:
        args += group
    args += belows
    return call(
        body,
        outs,
        args,
        24,
        [
            VMEM((harmonics, 2 * LANES), BF16),
            VMEM((LANES, (blocks + bands) * 2 * LANES), BF16),
        ],
    )


def sweep_layers(source, transfer, fields, orders):
    layers = lax.axis_size("layer")
    count = lax.axis_size("harm")
    harmonics = orders.shape[0]
    columns = source.shape[2]
    rows = source.shape[1]
    fan = rows % LANES == 0 and count == len(ORDER) and layers > 2
    band = 2 * harmonics // count
    scale = 1.0 / math.sqrt(harmonics * columns)
    axes = ("layer", "harm")
    top = layers - 1
    plan = routes(count) if fan else []
    still = list(range(count))

    def gathered(value):
        return [lax.all_gather(value, "harm", axis=1, tiled=True)]

    def to_layer(value, origins, target):
        if not fan:
            if origins[0] != target:
                pairs = [(origins[0] * count + h, target * count + h) for h in range(count)]
                value = lax.ppermute(value, axes, pairs)
            return gathered(value)
        out = []
        for origin, route in zip(origins, plan):
            if origin == target and route == still:
                out.append(value)
                continue
            pairs = [(origin * count + h, target * count + route[h]) for h in range(count)]
            out.append(lax.ppermute(value, axes, pairs))
        return out

    def in_layers(value, route):
        pairs = [(r * count + h, r * count + route[h]) for r in range(layers) for h in range(count)]
        return lax.ppermute(value, axes, pairs)

    matrix, own, table = bring(transfer[0], source, orders.reshape(1, harmonics))
    if fan:
        origins = [(s + 1) % (layers - 1) for s in range(count - 1)] + [top]
    else:
        origins = [top]
    shards = to_layer(source, origins, top)
    if fan:
        shards[-1] = own
    sets = [shards]
    belows = []
    mine = []
    for layer in range(top, 0, -1):
        below = propagate(matrix, shards, fan)
        belows.append(below)
        shards = to_layer(below, [layer] * count, layer - 1)
        sets.append(shards)
        if fan and layer == top:
            held, _ = lax.optimization_barrier((fields[0], below))
            beside = in_layers(held, [h ^ 1 for h in range(count)])
        if fan and layer == top - 1:
            pair, _ = lax.optimization_barrier((jnp.stack([fields[0], beside]), below))
            for name in FEED[:-1]:
                turn = QUARTERS[name]
                mine.append(in_layers(pair, [turn[h // 2] * 2 + h % 2 for h in range(count)]))
            mine.append(pair)
    if not fan:
        mine = gathered(fields[0])
    factors = sort_fields(table, mine, fan)
    grads, bottom = finish(
        matrix, table, factors, sets[::-1], belows[::-1], fan, band, scale
    )
    return grads, bottom


def solution(mesh):
    return jax.shard_map(
        sweep_layers,
        mesh=mesh,
        in_specs=(
            P(None, "harm", None),
            P("layer", None, "harm", None),
            P("layer", None, "harm", None),
            P(),
        ),
        out_specs=(P("layer", None, "harm"), P("layer", None, "harm", None)),
        check_vma=False,
    )
```

```python
import math

import jax
import jax.numpy as jnp
from jax import lax
from jax.experimental import pallas as pl
from jax.experimental.pallas import tpu as pltpu
from jax.sharding import PartitionSpec as P


LANES = 128
VMEM = pltpu.VMEM
BF16 = jnp.bfloat16
F32 = jnp.float32


def call(body, outs, args, limit, scratch=()):
    spec = pl.BlockSpec(memory_space=VMEM)
    return pl.pallas_call(
        body,
        out_shape=outs,
        in_specs=[spec] * len(args),
        out_specs=jax.tree.map(lambda _: spec, outs),
        scratch_shapes=list(scratch),
        compiler_params=pltpu.CompilerParams(vmem_limit_bytes=limit << 20),
    )(*[pltpu.with_memory_space_constraint(a, VMEM) for a in args])


def joined(value):
    return jnp.concatenate([value[0], value[1]], axis=1)


QUARTERS = {
    "far": (3, 2, 1, 0),
    "out": (1, 3, 0, 2),
    "in": (2, 0, 3, 1),
    "own": (0, 1, 2, 3),
}
FEED = ("far", "out", "in", "own")
ORDER = ("far0", "own1", "far1", "out0", "out1", "in0", "in1", "own0")


def routes(count):
    half = count // 4
    return [
        [QUARTERS[slot[:-1]][h // half] * half + (h % half ^ int(slot[-1])) for h in range(count)]
        for slot in ORDER
    ]


def partner(step, fan):
    if not fan:
        return 0
    targets = routes(lax.axis_size("harm"))[step]
    here = lax.axis_index("harm")
    origin = jnp.int32(targets.index(0))
    for spot in range(1, len(targets)):
        origin = jnp.where(here == spot, targets.index(spot), origin)
    return origin


def product(matrix_ref, shards, fan):
    rows = matrix_ref.shape[1]
    part = jnp.zeros((rows, 2 * LANES), F32)
    by_re, by_im = part, part
    for step, value in enumerate(shards):
        size = value.shape[1]
        start = pl.multiple_of(partner(step, fan) * size, size) if fan else 0
        cols = pl.ds(start, size)
        both = joined(value)
        by_re += jnp.dot(matrix_ref[0, :, cols], both, preferred_element_type=F32)
        by_im += jnp.dot(matrix_ref[1, :, cols], both, preferred_element_type=F32)
    re = by_re[:, :LANES] - by_im[:, LANES:]
    im = by_re[:, LANES:] + by_im[:, :LANES]
    return re.astype(BF16), im.astype(BF16)


def propagate(matrix, shards, fan):
    def body(matrix_ref, *refs):
        out_ref = refs[-1]
        re, im = product(matrix_ref, [r[...] for r in refs[:-1]], fan)
        out_ref[0] = re
        out_ref[1] = im

    rows = matrix.shape[1]
    return call(body, VMEM((2, rows, LANES), BF16), [matrix, *shards], 8)


def one_hot(targets, first, count):
    index = lax.broadcasted_iota(jnp.int32, (count, targets.shape[1]), 0) + first
    return jnp.where(index == targets, 1.0, 0.0).astype(BF16)


def bring(matrix, source, orders):
    args = [matrix, source, orders]

    def body(*refs):
        size = len(args)
        ins, outs, sems = refs[:size], refs[size : 2 * size], refs[-1]
        copies = [
            pltpu.make_async_copy(ins[i], outs[i], sems.at[i]) for i in range(size)
        ]
        for copy in copies:
            copy.start()
        for copy in copies:
            copy.wait()

    hbm = pl.BlockSpec(memory_space=pltpu.HBM)
    return pl.pallas_call(
        body,
        out_shape=[VMEM(a.shape, a.dtype) for a in args],
        in_specs=[hbm] * len(args),
        out_specs=[pl.BlockSpec(memory_space=VMEM)] * len(args),
        scratch_shapes=[pltpu.SemaphoreType.DMA((len(args),))],
        compiler_params=pltpu.CompilerParams(vmem_limit_bytes=1 << 20),
        name="bring",
    )(*[pltpu.with_memory_space_constraint(a, pltpu.HBM) for a in args])


def sort_fields(orders, shards, fan, split):
    harmonics = orders.shape[1]
    blocks = harmonics // LANES

    def body(orders_ref, *refs):
        shard_refs, out_ref, whole = refs[:-2], refs[-2], refs[-1]
        if fan:
            here = lax.axis_index("harm")
            low = lax.axis_index("layer") < split
            moves = len(FEED) - 1
            for place, name in enumerate(FEED):
                quarter = jnp.int32(QUARTERS[name].index(0))
                for spot in range(1, 4):
                    quarter = jnp.where(here // 2 == spot, QUARTERS[name].index(spot), quarter)
                size = shard_refs[-1].shape[2]
                for part in range(2):
                    value = shard_refs[-1][part]
                    if place < moves:
                        value = jnp.where(
                            low, shard_refs[place][part], shard_refs[moves + place][part]
                        )
                    start = (quarter * 2 + (here % 2 ^ part)) * size
                    put(whole, pl.multiple_of(start, size), value)
        else:
            put(whole, 0, shard_refs[0][...])
        targets = orders_ref[...] ^ (LANES - 1)
        chunk = 4 * LANES

        def step(c, carry):
            picked = jnp.dot(
                one_hot(targets, c * chunk, chunk), whole[...], preferred_element_type=F32
            ).astype(BF16)
            for b in range(chunk // LANES):
                re = picked[b * LANES : (b + 1) * LANES, :LANES]
                im = picked[b * LANES : (b + 1) * LANES, LANES:]
                at = pl.multiple_of((c * (chunk // LANES) + b) * 2 * LANES, LANES)
                out_ref[:LANES, pl.ds(at, LANES)] = re
                out_ref[:LANES, pl.ds(at + LANES, LANES)] = -im
                out_ref[LANES:, pl.ds(at, LANES)] = im
                out_ref[LANES:, pl.ds(at + LANES, LANES)] = re
            return carry

        lax.fori_loop(0, harmonics // chunk, step, 0)

    return call(
        body,
        VMEM((2 * LANES, blocks * 2 * LANES), BF16),
        [orders, *shards],
        24,
        [VMEM((harmonics, 2 * LANES), BF16)],
    )


def put(whole, start, value):
    rows = pl.ds(start, value.shape[1])
    whole[rows, :LANES] = value[0]
    whole[rows, LANES:] = value[1]


def fill(whole, shards, fan):
    for step, value in enumerate(shards):
        size = value.shape[1]
        start = pl.multiple_of(partner(step, fan) * size, size) if fan else 0
        put(whole, start, value)


def finish(matrix, orders, factors, sets, belows, fan, band, scale):
    layers = len(sets)
    harmonics = orders.shape[1]
    rows = matrix.shape[1]
    blocks = harmonics // LANES
    bands = band // LANES
    strip = bands + 1
    per_set = [len(s) for s in sets]

    def body(matrix_ref, orders_ref, factors_ref, *refs):
        refs = list(refs)
        set_refs = []
        for count in per_set:
            set_refs.append(refs[:count])
            refs = refs[count:]
        below_refs, refs = refs[: layers - 1], refs[layers - 1 :]
        grad_ref, bottom_ref, whole, moved = refs
        layer = lax.axis_index("layer")
        last = [r[...] for r in set_refs[0]]
        chosen = last
        for index in range(1, layers):
            chosen = [
                jnp.where(layer == index, r[...], c) for r, c in zip(set_refs[index], chosen)
            ]
        fill(whole, chosen, fan)
        re, im = product(matrix_ref, last, fan)
        for index in range(1, layers):
            re = jnp.where(layer == index, below_refs[index - 1][0], re)
            im = jnp.where(layer == index, below_refs[index - 1][1], im)
        bottom_ref[0, 0] = re
        bottom_ref[0, 1] = im

        targets = orders_ref[...] + (harmonics - 1 - band * lax.axis_index("harm"))
        for c in range(blocks + bands):
            picked = jnp.dot(
                one_hot(targets, c * LANES, LANES), whole[...], preferred_element_type=F32
            ).astype(BF16)
            moved[:, c * 2 * LANES : (c + 1) * 2 * LANES] = picked
        width = 2 * LANES
        length = blocks * width
        parts = []
        for q in range(strip):
            parts.append(
                lax.dot_general(
                    factors_ref[...],
                    moved[:, q * width : q * width + length],
                    (((1,), (1,)), ((), ())),
                    preferred_element_type=F32,
                )
            )
        strips = jnp.concatenate(parts, axis=1)
        size = strip * LANES
        for part in range(2):
            skewed = pltpu.roll(
                strips[part * LANES : (part + 1) * LANES],
                size - (LANES - 1),
                1,
                stride=1,
                stride_axis=0,
            )
            total = jnp.sum(skewed[:, :band], axis=0, keepdims=True) * scale
            grad_ref[0, pl.ds(part, 1), :] = total

    outs = (
        jax.ShapeDtypeStruct((1, 2, band), F32),
        jax.ShapeDtypeStruct((1, 2, rows, LANES), BF16),
    )
    args = [matrix, orders, factors]
    for group in sets:
        args += group
    args += belows
    return call(
        body,
        outs,
        args,
        24,
        [
            VMEM((harmonics, 2 * LANES), BF16),
            VMEM((LANES, (blocks + bands) * 2 * LANES), BF16),
        ],
    )


def sweep_layers(source, transfer, fields, orders):
    layers = lax.axis_size("layer")
    count = lax.axis_size("harm")
    harmonics = orders.shape[0]
    columns = source.shape[2]
    rows = source.shape[1]
    fan = rows % LANES == 0 and count == len(ORDER) and layers > 2
    band = 2 * harmonics // count
    scale = 1.0 / math.sqrt(harmonics * columns)
    axes = ("layer", "harm")
    top = layers - 1
    plan = routes(count) if fan else []
    still = list(range(count))

    def gathered(value):
        return [lax.all_gather(value, "harm", axis=1, tiled=True)]

    def to_layer(value, origins, target):
        if not fan:
            if origins[0] != target:
                pairs = [(origins[0] * count + h, target * count + h) for h in range(count)]
                value = lax.ppermute(value, axes, pairs)
            return gathered(value)
        out = []
        for origin, route in zip(origins, plan):
            if origin == target and route == still:
                out.append(value)
                continue
            pairs = [(origin * count + h, target * count + route[h]) for h in range(count)]
            out.append(lax.ppermute(value, axes, pairs))
        return out

    def in_layers(value, members, route):
        pairs = [(r * count + h, r * count + route[h]) for r in members for h in range(count)]
        if min(members) == 0 and max(members) < top:
            spare = (max(members) + 1) * count
            pairs.append((spare, spare))
        return lax.ppermute(value, axes, pairs)

    def along(value, members):
        return [
            in_layers(value, members, [QUARTERS[name][h // 2] * 2 + h % 2 for h in range(count)])
            for name in FEED[:-1]
        ]

    matrix, own, table = bring(transfer[0], source, orders.reshape(1, harmonics))
    if fan:
        origins = [(s + 1) % (layers - 1) for s in range(count - 1)] + [top]
    else:
        origins = [top]
    shards = to_layer(source, origins, top)
    split = layers // 2
    if fan:
        shards[-1] = own
        beside = in_layers(fields[0], range(layers), [h ^ 1 for h in range(count)])
    sets = [shards]
    belows = []
    mine = []
    for layer in range(top, 0, -1):
        below = propagate(matrix, shards, fan)
        belows.append(below)
        shards = to_layer(below, [layer] * count, layer - 1)
        sets.append(shards)
        if fan and layer == top:
            beside, _ = lax.optimization_barrier((beside, below))
            pair = jnp.stack([fields[0], beside])
            mine += along(pair, range(split))
        if fan and layer == top - 1:
            held, _ = lax.optimization_barrier((pair, below))
            mine += along(held, range(split, layers))
            mine.append(held)
    if not fan:
        mine = gathered(fields[0])
    factors = sort_fields(table, mine, fan, split)
    grads, bottom = finish(
        matrix, table, factors, sets[::-1], belows[::-1], fan, band, scale
    )
    return grads, bottom


def solution(mesh):
    return jax.shard_map(
        sweep_layers,
        mesh=mesh,
        in_specs=(
            P(None, "harm", None),
            P("layer", None, "harm", None),
            P("layer", None, "harm", None),
            P(),
        ),
        out_specs=(P("layer", None, "harm"), P("layer", None, "harm", None)),
        check_vma=False,
    )
```

```python
import math

import jax
import jax.numpy as jnp
from jax import lax
from jax.experimental import pallas as pl
from jax.experimental.pallas import tpu as pltpu
from jax.sharding import PartitionSpec as P


LANES = 128
VMEM = pltpu.VMEM
BF16 = jnp.bfloat16
F32 = jnp.float32

QUARTERS = {
    "far": (3, 2, 1, 0),
    "out": (1, 3, 0, 2),
    "in": (2, 0, 3, 1),
    "own": (0, 1, 2, 3),
}
ORDER = ("far0", "own1", "far1", "out0", "out1", "in0", "in1", "own0")
WHOLE = "all"


def route(slot):
    turn, swap = QUARTERS[slot[:-1]], int(slot[-1])
    half = len(ORDER) // len(turn)
    return [turn[h // half] * half + (h % half ^ swap) for h in range(len(ORDER))]


def place(slot, size):
    if slot == WHOLE:
        return 0
    targets = route(slot)
    here = lax.axis_index("harm")
    start = jnp.int32(targets.index(0) * size)
    for spot in range(1, len(targets)):
        start = jnp.where(here == spot, targets.index(spot) * size, start)
    return pl.multiple_of(start, size)


def listed(*sets):
    arrays, maps = [], []
    for group in sets:
        found = {}
        for slot, (value, part) in group.items():
            spot = next((i for i, a in enumerate(arrays) if a is value), len(arrays))
            if spot == len(arrays):
                arrays.append(value)
            found[slot] = (spot, part)
        maps.append(found)
    return arrays, maps


def read(refs, entry):
    spot, part = entry
    return refs[spot][...] if part is None else refs[spot][part]


def call(body, outs, args, limit, scratch=()):
    spec = pl.BlockSpec(memory_space=VMEM)
    return pl.pallas_call(
        body,
        out_shape=outs,
        in_specs=[spec] * len(args),
        out_specs=jax.tree.map(lambda _: spec, outs),
        scratch_shapes=list(scratch),
        compiler_params=pltpu.CompilerParams(vmem_limit_bytes=limit << 20),
    )(*[pltpu.with_memory_space_constraint(a, VMEM) for a in args])


def product(matrix_ref, pieces):
    rows = matrix_ref.shape[1]
    part = jnp.zeros((rows, 2 * LANES), F32)
    by_re, by_im = part, part
    for slot, value in pieces.items():
        size = value.shape[1]
        cols = pl.ds(place(slot, size), size)
        both = jnp.concatenate([value[0], value[1]], axis=1)
        by_re += jnp.dot(matrix_ref[0, :, cols], both, preferred_element_type=F32)
        by_im += jnp.dot(matrix_ref[1, :, cols], both, preferred_element_type=F32)
    re = by_re[:, :LANES] - by_im[:, LANES:]
    im = by_re[:, LANES:] + by_im[:, :LANES]
    return re.astype(BF16), im.astype(BF16)


def propagate(matrix, group):
    arrays, (spots,) = listed(group)

    def body(matrix_ref, *refs):
        out_ref = refs[-1]
        re, im = product(matrix_ref, {slot: read(refs, e) for slot, e in spots.items()})
        out_ref[0] = re
        out_ref[1] = im

    rows = matrix.shape[1]
    return call(body, VMEM((2, rows, LANES), BF16), [matrix, *arrays], 8)


def one_hot(targets, first, count):
    index = lax.broadcasted_iota(jnp.int32, (count, targets.shape[1]), 0) + first
    return jnp.where(index == targets, 1.0, 0.0).astype(BF16)


def fill(whole, pieces):
    for slot, value in pieces.items():
        rows = pl.ds(place(slot, value.shape[1]), value.shape[1])
        whole[rows, :LANES] = value[0]
        whole[rows, LANES:] = value[1]


def bring(matrix, source, orders):
    args = [matrix, source, orders]

    def body(*refs):
        size = len(args)
        ins, outs, sems = refs[:size], refs[size : 2 * size], refs[-1]
        copies = [
            pltpu.make_async_copy(ins[i], outs[i], sems.at[i]) for i in range(size)
        ]
        for copy in copies:
            copy.start()
        for copy in copies:
            copy.wait()

    hbm = pl.BlockSpec(memory_space=pltpu.HBM)
    return pl.pallas_call(
        body,
        out_shape=[VMEM(a.shape, a.dtype) for a in args],
        in_specs=[hbm] * len(args),
        out_specs=[pl.BlockSpec(memory_space=VMEM)] * len(args),
        scratch_shapes=[pltpu.SemaphoreType.DMA((len(args),))],
        compiler_params=pltpu.CompilerParams(vmem_limit_bytes=1 << 20),
        name="bring",
    )(*[pltpu.with_memory_space_constraint(a, pltpu.HBM) for a in args])


def sort_fields(orders, low, high, split):
    harmonics = orders.shape[1]
    blocks = harmonics // LANES
    arrays, (low_spots, high_spots) = listed(low, high)

    def body(orders_ref, *refs):
        out_ref, whole = refs[-2:]
        lower = lax.axis_index("layer") < split
        pieces = {}
        for slot, entry in low_spots.items():
            pieces[slot] = read(refs, entry)
            if high_spots[slot] != entry:
                pieces[slot] = jnp.where(lower, pieces[slot], read(refs, high_spots[slot]))
        fill(whole, pieces)
        targets = orders_ref[...] ^ (LANES - 1)
        chunk = 4 * LANES

        def step(c, carry):
            picked = jnp.dot(
                one_hot(targets, c * chunk, chunk), whole[...], preferred_element_type=F32
            ).astype(BF16)
            for b in range(chunk // LANES):
                re = picked[b * LANES : (b + 1) * LANES, :LANES]
                im = picked[b * LANES : (b + 1) * LANES, LANES:]
                at = pl.multiple_of((c * (chunk // LANES) + b) * 2 * LANES, LANES)
                out_ref[:LANES, pl.ds(at, LANES)] = re
                out_ref[:LANES, pl.ds(at + LANES, LANES)] = -im
                out_ref[LANES:, pl.ds(at, LANES)] = im
                out_ref[LANES:, pl.ds(at + LANES, LANES)] = re
            return carry

        lax.fori_loop(0, harmonics // chunk, step, 0)

    return call(
        body,
        VMEM((2 * LANES, blocks * 2 * LANES), BF16),
        [orders, *arrays],
        24,
        [VMEM((harmonics, 2 * LANES), BF16)],
    )


def finish(matrix, orders, factors, sets, belows, band, scale):
    layers = len(sets)
    harmonics = orders.shape[1]
    rows = matrix.shape[1]
    blocks = harmonics // LANES
    bands = band // LANES
    strip = bands + 1
    arrays, maps = listed(*sets)

    def body(matrix_ref, orders_ref, factors_ref, *refs):
        set_refs, refs = refs[: len(arrays)], refs[len(arrays) :]
        below_refs, refs = refs[: layers - 1], refs[layers - 1 :]
        grad_ref, bottom_ref, whole, moved = refs
        layer = lax.axis_index("layer")
        last = {slot: read(set_refs, e) for slot, e in maps[0].items()}
        chosen = dict(last)
        for index in range(1, layers):
            for slot, entry in maps[index].items():
                chosen[slot] = jnp.where(layer == index, read(set_refs, entry), chosen[slot])
        fill(whole, chosen)
        re, im = product(matrix_ref, last)
        for index in range(1, layers):
            re = jnp.where(layer == index, below_refs[index - 1][0], re)
            im = jnp.where(layer == index, below_refs[index - 1][1], im)
        bottom_ref[0, 0] = re
        bottom_ref[0, 1] = im

        targets = orders_ref[...] + (harmonics - 1 - band * lax.axis_index("harm"))
        for c in range(blocks + bands):
            picked = jnp.dot(
                one_hot(targets, c * LANES, LANES), whole[...], preferred_element_type=F32
            ).astype(BF16)
            moved[:, c * 2 * LANES : (c + 1) * 2 * LANES] = picked
        width = 2 * LANES
        length = blocks * width
        parts = []
        for q in range(strip):
            parts.append(
                lax.dot_general(
                    factors_ref[...],
                    moved[:, q * width : q * width + length],
                    (((1,), (1,)), ((), ())),
                    preferred_element_type=F32,
                )
            )
        strips = jnp.concatenate(parts, axis=1)
        size = strip * LANES
        for part in range(2):
            skewed = pltpu.roll(
                strips[part * LANES : (part + 1) * LANES],
                size - (LANES - 1),
                1,
                stride=1,
                stride_axis=0,
            )
            total = jnp.sum(skewed[:, :band], axis=0, keepdims=True) * scale
            grad_ref[0, pl.ds(part, 1), :] = total

    outs = (
        jax.ShapeDtypeStruct((1, 2, band), F32),
        jax.ShapeDtypeStruct((1, 2, rows, LANES), BF16),
    )
    return call(
        body,
        outs,
        [matrix, orders, factors, *arrays, *belows],
        24,
        [
            VMEM((harmonics, 2 * LANES), BF16),
            VMEM((LANES, (blocks + bands) * 2 * LANES), BF16),
        ],
    )


def sweep(*args):
    layers, count = lax.axis_size("layer"), lax.axis_size("harm")
    if layers > 2 and count == len(ORDER) and args[0].shape[1] % LANES == 0:
        return direct_sweep(*args)
    return gather_sweep(*args)


def sizes(source, orders):
    harmonics = orders.shape[0]
    band = 2 * harmonics // lax.axis_size("harm")
    return band, 1.0 / math.sqrt(harmonics * source.shape[2])


def gather_sweep(source, transfer, fields, orders):
    layers, count = lax.axis_size("layer"), lax.axis_size("harm")
    band, scale = sizes(source, orders)

    def gathered(value):
        return {WHOLE: (lax.all_gather(value, "harm", axis=1, tiled=True), None)}

    matrix, _, table = bring(transfer[0], source, orders.reshape(1, -1))
    group = gathered(source)
    sets, belows = [group], []
    for layer in range(layers - 1, 0, -1):
        below = propagate(matrix, group)
        pairs = [(layer * count + h, (layer - 1) * count + h) for h in range(count)]
        group = gathered(lax.ppermute(below, ("layer", "harm"), pairs))
        sets.append(group)
        belows.append(below)
    held = gathered(fields[0])
    factors = sort_fields(table, held, held, layers)
    return finish(matrix, table, factors, sets[::-1], belows[::-1], band, scale)


def direct_sweep(source, transfer, fields, orders):
    layers, count = lax.axis_size("layer"), lax.axis_size("harm")
    band, scale = sizes(source, orders)
    top = layers - 1
    split = layers // 2

    def move(value, origin, target, slot):
        pairs = [(origin * count + h, target * count + t) for h, t in enumerate(route(slot))]
        return lax.ppermute(value, ("layer", "harm"), pairs)

    def among(value, members, slot):
        pairs = [
            (r * count + h, r * count + t) for r in members for h, t in enumerate(route(slot))
        ]
        return lax.ppermute(value, ("layer", "harm"), pairs)

    def along(pair, members):
        group = {"own0": (pair, 0), "own1": (pair, 1)}
        for name in ("far", "out", "in"):
            got = among(pair, members, name + "0")
            group[name + "0"] = (got, 0)
            group[name + "1"] = (got, 1)
        return group

    matrix, own, table = bring(transfer[0], source, orders.reshape(1, -1))
    group = {}
    for step, slot in enumerate(("far0", "far1", "out0", "out1")):
        group[slot] = (move(source, (step + 1) % top, top, slot), None)
    both = among(jnp.stack([fields[0], source]), range(layers), "own1")
    group["own1"] = (both, 1)
    got = move(jnp.stack([source, both[1]]), 0, top, "in0")
    group["in0"] = (got, 0)
    group["in1"] = (got, 1)
    group["own0"] = (own, None)
    pair = jnp.stack([fields[0], both[0]])
    low = along(pair, range(split))

    sets, belows = [group], []
    for layer in range(top, 0, -1):
        below = propagate(matrix, group)
        group = {}
        for slot in ORDER:
            group[slot] = (move(below, layer, layer - 1, slot), None)
        sets.append(group)
        belows.append(below)
        if layer == top - 1:
            held, _ = lax.optimization_barrier((pair, below))
            high = along(held, range(split, layers))
    for slot in ("own0", "own1"):
        low[slot] = high[slot]
    factors = sort_fields(table, low, high, split)
    return finish(matrix, table, factors, sets[::-1], belows[::-1], band, scale)


def solution(mesh):
    return jax.shard_map(
        sweep,
        mesh=mesh,
        in_specs=(
            P(None, "harm", None),
            P("layer", None, "harm", None),
            P("layer", None, "harm", None),
            P(),
        ),
        out_specs=(P("layer", None, "harm"), P("layer", None, "harm", None)),
        check_vma=False,
    )
```

```python
import math

import jax
import jax.numpy as jnp
from jax import lax
from jax.experimental import pallas as pl
from jax.experimental.pallas import tpu as pltpu
from jax.sharding import PartitionSpec as P


LANES = 128
VMEM = pltpu.VMEM
BF16 = jnp.bfloat16
F32 = jnp.float32

QUARTERS = {
    "far": (3, 2, 1, 0),
    "out": (1, 3, 0, 2),
    "in": (2, 0, 3, 1),
    "own": (0, 1, 2, 3),
}
ORDER = ("far0", "own1", "far1", "out0", "out1", "in0", "in1", "own0")
TURNS = ("far", "out", "in")
WHOLE = "all"


def route(slot):
    turn, swap = QUARTERS[slot[:-1]], int(slot[-1])
    half = len(ORDER) // len(turn)
    return [turn[h // half] * half + (h % half ^ swap) for h in range(len(ORDER))]


def place(slot, size):
    if slot == WHOLE:
        return 0
    targets = route(slot)
    here = lax.axis_index("harm")
    start = jnp.int32(targets.index(0) * size)
    for spot in range(1, len(targets)):
        start = jnp.where(here == spot, targets.index(spot) * size, start)
    return pl.multiple_of(start, size)


def listed(*sets):
    arrays, maps = [], []
    for group in sets:
        found = {}
        for slot, (value, part) in group.items():
            spot = next((i for i, a in enumerate(arrays) if a is value), len(arrays))
            if spot == len(arrays):
                arrays.append(value)
            found[slot] = (spot, part)
        maps.append(found)
    return arrays, maps


def read(refs, entry):
    spot, part = entry
    return refs[spot][...] if part is None else refs[spot][part]


def call(body, outs, args, limit, scratch=()):
    spec = pl.BlockSpec(memory_space=VMEM)
    return pl.pallas_call(
        body,
        out_shape=outs,
        in_specs=[spec] * len(args),
        out_specs=jax.tree.map(lambda _: spec, outs),
        scratch_shapes=list(scratch),
        compiler_params=pltpu.CompilerParams(vmem_limit_bytes=limit << 20),
    )(*[pltpu.with_memory_space_constraint(a, VMEM) for a in args])


def product(matrix_ref, pieces):
    rows = matrix_ref.shape[1]
    part = jnp.zeros((rows, 2 * LANES), F32)
    by_re, by_im = part, part
    for slot, value in pieces.items():
        size = value.shape[1]
        cols = pl.ds(place(slot, size), size)
        both = jnp.concatenate([value[0], value[1]], axis=1)
        by_re += jnp.dot(matrix_ref[0, :, cols], both, preferred_element_type=F32)
        by_im += jnp.dot(matrix_ref[1, :, cols], both, preferred_element_type=F32)
    re = by_re[:, :LANES] - by_im[:, LANES:]
    im = by_re[:, LANES:] + by_im[:, :LANES]
    return re.astype(BF16), im.astype(BF16)


def propagate(matrix, group):
    arrays, (spots,) = listed(group)

    def body(matrix_ref, *refs):
        out_ref = refs[-1]
        re, im = product(matrix_ref, {slot: read(refs, e) for slot, e in spots.items()})
        out_ref[0] = re
        out_ref[1] = im

    rows = matrix.shape[1]
    return call(body, VMEM((2, rows, LANES), BF16), [matrix, *arrays], 8)


def one_hot(targets, first, count):
    index = lax.broadcasted_iota(jnp.int32, (count, targets.shape[1]), 0) + first
    return jnp.where(index == targets, 1.0, 0.0).astype(BF16)


def fill(whole, pieces):
    for slot, value in pieces.items():
        rows = pl.ds(place(slot, value.shape[1]), value.shape[1])
        whole[rows, :LANES] = value[0]
        whole[rows, LANES:] = value[1]


def bring(matrix, source, orders):
    args = [matrix, source, orders]

    def body(*refs):
        size = len(args)
        ins, outs, sems = refs[:size], refs[size : 2 * size], refs[-1]
        copies = [
            pltpu.make_async_copy(ins[i], outs[i], sems.at[i]) for i in range(size)
        ]
        for copy in copies:
            copy.start()
        for copy in copies:
            copy.wait()

    hbm = pl.BlockSpec(memory_space=pltpu.HBM)
    return pl.pallas_call(
        body,
        out_shape=[VMEM(a.shape, a.dtype) for a in args],
        in_specs=[hbm] * len(args),
        out_specs=[pl.BlockSpec(memory_space=VMEM)] * len(args),
        scratch_shapes=[pltpu.SemaphoreType.DMA((len(args),))],
        compiler_params=pltpu.CompilerParams(vmem_limit_bytes=1 << 20),
        name="bring",
    )(*[pltpu.with_memory_space_constraint(a, pltpu.HBM) for a in args])


def sort_fields(orders, held):
    harmonics = orders.shape[1]
    blocks = harmonics // LANES
    arrays, (spots,) = listed(held)

    def body(orders_ref, *refs):
        out_ref, whole = refs[-2:]
        fill(whole, {slot: read(refs, e) for slot, e in spots.items()})
        targets = orders_ref[...] ^ (LANES - 1)
        chunk = 4 * LANES

        def step(c, carry):
            picked = jnp.dot(
                one_hot(targets, c * chunk, chunk), whole[...], preferred_element_type=F32
            ).astype(BF16)
            for b in range(chunk // LANES):
                re = picked[b * LANES : (b + 1) * LANES, :LANES]
                im = picked[b * LANES : (b + 1) * LANES, LANES:]
                at = pl.multiple_of((c * (chunk // LANES) + b) * 2 * LANES, LANES)
                out_ref[:LANES, pl.ds(at, LANES)] = re
                out_ref[:LANES, pl.ds(at + LANES, LANES)] = -im
                out_ref[LANES:, pl.ds(at, LANES)] = im
                out_ref[LANES:, pl.ds(at + LANES, LANES)] = re
            return carry

        lax.fori_loop(0, harmonics // chunk, step, 0)

    return call(
        body,
        VMEM((2 * LANES, blocks * 2 * LANES), BF16),
        [orders, *arrays],
        24,
        [VMEM((harmonics, 2 * LANES), BF16)],
    )


def finish(matrix, orders, factors, sets, belows, band, scale):
    layers = len(sets)
    harmonics = orders.shape[1]
    rows = matrix.shape[1]
    blocks = harmonics // LANES
    bands = band // LANES
    strip = bands + 1
    arrays, maps = listed(*sets)

    def body(matrix_ref, orders_ref, factors_ref, *refs):
        set_refs, refs = refs[: len(arrays)], refs[len(arrays) :]
        below_refs, refs = refs[: layers - 1], refs[layers - 1 :]
        grad_ref, bottom_ref, whole, moved = refs
        layer = lax.axis_index("layer")
        last = {slot: read(set_refs, e) for slot, e in maps[0].items()}
        chosen = dict(last)
        for index in range(1, layers):
            for slot, entry in maps[index].items():
                chosen[slot] = jnp.where(layer == index, read(set_refs, entry), chosen[slot])
        fill(whole, chosen)
        re, im = product(matrix_ref, last)
        for index in range(1, layers):
            re = jnp.where(layer == index, below_refs[index - 1][0], re)
            im = jnp.where(layer == index, below_refs[index - 1][1], im)
        bottom_ref[0, 0] = re
        bottom_ref[0, 1] = im

        targets = orders_ref[...] + (harmonics - 1 - band * lax.axis_index("harm"))
        for c in range(blocks + bands):
            picked = jnp.dot(
                one_hot(targets, c * LANES, LANES), whole[...], preferred_element_type=F32
            ).astype(BF16)
            moved[:, c * 2 * LANES : (c + 1) * 2 * LANES] = picked
        width = 2 * LANES
        length = blocks * width
        parts = []
        for q in range(strip):
            parts.append(
                lax.dot_general(
                    factors_ref[...],
                    moved[:, q * width : q * width + length],
                    (((1,), (1,)), ((), ())),
                    preferred_element_type=F32,
                )
            )
        strips = jnp.concatenate(parts, axis=1)
        size = strip * LANES
        for part in range(2):
            skewed = pltpu.roll(
                strips[part * LANES : (part + 1) * LANES],
                size - (LANES - 1),
                1,
                stride=1,
                stride_axis=0,
            )
            total = jnp.sum(skewed[:, :band], axis=0, keepdims=True) * scale
            grad_ref[0, pl.ds(part, 1), :] = total

    outs = (
        jax.ShapeDtypeStruct((1, 2, band), F32),
        jax.ShapeDtypeStruct((1, 2, rows, LANES), BF16),
    )
    return call(
        body,
        outs,
        [matrix, orders, factors, *arrays, *belows],
        24,
        [
            VMEM((harmonics, 2 * LANES), BF16),
            VMEM((LANES, (blocks + bands) * 2 * LANES), BF16),
        ],
    )


def sweep(*args):
    layers, count = lax.axis_size("layer"), lax.axis_size("harm")
    if layers > 2 and count == len(ORDER) and args[0].shape[1] % LANES == 0:
        return direct_sweep(*args)
    return gather_sweep(*args)


def sizes(source, orders):
    harmonics = orders.shape[0]
    band = 2 * harmonics // lax.axis_size("harm")
    return band, 1.0 / math.sqrt(harmonics * source.shape[2])


def gather_sweep(source, transfer, fields, orders):
    layers, count = lax.axis_size("layer"), lax.axis_size("harm")
    band, scale = sizes(source, orders)

    def gathered(value):
        return {WHOLE: (lax.all_gather(value, "harm", axis=1, tiled=True), None)}

    matrix, _, table = bring(transfer[0], source, orders.reshape(1, -1))
    group = gathered(source)
    sets, belows = [group], []
    for layer in range(layers - 1, 0, -1):
        below = propagate(matrix, group)
        pairs = [(layer * count + h, (layer - 1) * count + h) for h in range(count)]
        group = gathered(lax.ppermute(below, ("layer", "harm"), pairs))
        sets.append(group)
        belows.append(below)
    factors = sort_fields(table, gathered(fields[0]))
    return finish(matrix, table, factors, sets[::-1], belows[::-1], band, scale)


def direct_sweep(source, transfer, fields, orders):
    layers, count = lax.axis_size("layer"), lax.axis_size("harm")
    band, scale = sizes(source, orders)
    top = layers - 1
    split = layers // 2

    def move(value, origin, target, slot):
        pairs = [(origin * count + h, target * count + t) for h, t in enumerate(route(slot))]
        return lax.ppermute(value, ("layer", "harm"), pairs)

    def among(value, members, slot):
        pairs = [
            (r * count + h, r * count + t) for r in members for h, t in enumerate(route(slot))
        ]
        return lax.ppermute(value, ("layer", "harm"), pairs)

    matrix, own, table = bring(transfer[0], source, orders.reshape(1, -1))
    group = {"own0": (own, None)}
    for slot in ORDER[:-1]:
        origin = top - 1 if slot[-1] == "1" and slot != "own1" else len(group) % split
        group[slot] = (move(source, origin, top, slot), None)
    along = [among(fields[0], range(layers), turn + "0") for turn in TURNS]

    sets, belows = [group], []
    for layer in range(top, 0, -1):
        below = propagate(matrix, group)
        group = {}
        for slot in ORDER:
            group[slot] = (move(below, layer, layer - 1, slot), None)
        sets.append(group)
        belows.append(below)
        if layer == top - 1:
            along, _ = lax.optimization_barrier((along, below))
            mine = jnp.stack([*along, fields[0]])
            beside = among(mine, range(layers), "own1")
    held = {}
    for part, turn in enumerate((*TURNS, "own")):
        held[turn + "0"] = (mine, part)
        held[turn + "1"] = (beside, part)
    factors = sort_fields(table, held)
    return finish(matrix, table, factors, sets[::-1], belows[::-1], band, scale)


def solution(mesh):
    return jax.shard_map(
        sweep,
        mesh=mesh,
        in_specs=(
            P(None, "harm", None),
            P("layer", None, "harm", None),
            P("layer", None, "harm", None),
            P(),
        ),
        out_specs=(P("layer", None, "harm"), P("layer", None, "harm", None)),
        check_vma=False,
    )
```

```python
import math

import jax
import jax.numpy as jnp
from jax import lax
from jax.experimental import pallas as pl
from jax.experimental.pallas import tpu as pltpu
from jax.sharding import PartitionSpec as P


LANES = 128
VMEM = pltpu.VMEM
BF16 = jnp.bfloat16
F32 = jnp.float32

QUARTERS = {
    "far": (3, 2, 1, 0),
    "out": (1, 3, 0, 2),
    "in": (2, 0, 3, 1),
    "own": (0, 1, 2, 3),
}
ORDER = ("far0", "own1", "far1", "out0", "out1", "in0", "in1", "own0")
EARLY, LATE = list(ORDER[:4]), list(ORDER[4:])
TURNS = ("far", "out", "in")
WHOLE = "all"


def route(slot):
    turn, swap = QUARTERS[slot[:-1]], int(slot[-1])
    half = len(ORDER) // len(turn)
    return [turn[h // half] * half + (h % half ^ swap) for h in range(len(ORDER))]


def place(slot, size):
    if slot == WHOLE:
        return 0
    targets = route(slot)
    here = lax.axis_index("harm")
    start = jnp.int32(targets.index(0) * size)
    for spot in range(1, len(targets)):
        start = jnp.where(here == spot, targets.index(spot) * size, start)
    return pl.multiple_of(start, size)


def listed(*sets):
    arrays, maps = [], []
    for group in sets:
        found = {}
        for slot, (value, part) in group.items():
            spot = next((i for i, a in enumerate(arrays) if a is value), len(arrays))
            if spot == len(arrays):
                arrays.append(value)
            found[slot] = (spot, part)
        maps.append(found)
    return arrays, maps


def read(refs, entry):
    spot, part = entry
    return refs[spot][...] if part is None else refs[spot][part]


def call(body, outs, args, limit, scratch=()):
    spec = pl.BlockSpec(memory_space=VMEM)
    return pl.pallas_call(
        body,
        out_shape=outs,
        in_specs=[spec] * len(args),
        out_specs=jax.tree.map(lambda _: spec, outs),
        scratch_shapes=list(scratch),
        compiler_params=pltpu.CompilerParams(vmem_limit_bytes=limit << 20),
    )(*[pltpu.with_memory_space_constraint(a, VMEM) for a in args])


def partial_product(matrix_ref, pieces, sums):
    by_re, by_im = sums
    for slot, value in pieces.items():
        size = value.shape[1]
        cols = pl.ds(place(slot, size), size)
        both = jnp.concatenate([value[0], value[1]], axis=1)
        by_re += jnp.dot(matrix_ref[0, :, cols], both, preferred_element_type=F32)
        by_im += jnp.dot(matrix_ref[1, :, cols], both, preferred_element_type=F32)
    return by_re, by_im


def zeros(matrix_ref):
    part = jnp.zeros((matrix_ref.shape[1], 2 * LANES), F32)
    return part, part


def complex_product(sums):
    by_re, by_im = sums
    re = by_re[:, :LANES] - by_im[:, LANES:]
    im = by_re[:, LANES:] + by_im[:, :LANES]
    return re.astype(BF16), im.astype(BF16)


def propagate(matrix, group):
    arrays, (spots,) = listed(group)

    def body(matrix_ref, *refs):
        out_ref = refs[-1]
        pieces = {slot: read(refs, e) for slot, e in spots.items()}
        re, im = complex_product(partial_product(matrix_ref, pieces, zeros(matrix_ref)))
        out_ref[0] = re
        out_ref[1] = im

    rows = matrix.shape[1]
    return call(body, VMEM((2, rows, LANES), BF16), [matrix, *arrays], 8)


def one_hot(targets, first, count):
    index = lax.broadcasted_iota(jnp.int32, (count, targets.shape[1]), 0) + first
    return jnp.where(index == targets, 1.0, 0.0).astype(BF16)


def fill(whole, pieces):
    for slot, value in pieces.items():
        rows = pl.ds(place(slot, value.shape[1]), value.shape[1])
        whole[rows, :LANES] = value[0]
        whole[rows, LANES:] = value[1]


def bring(matrix, source, orders):
    args = [matrix, source, orders]

    def body(*refs):
        size = len(args)
        ins, outs, sems = refs[:size], refs[size : 2 * size], refs[-1]
        copies = [
            pltpu.make_async_copy(ins[i], outs[i], sems.at[i]) for i in range(size)
        ]
        for copy in copies:
            copy.start()
        for copy in copies:
            copy.wait()

    hbm = pl.BlockSpec(memory_space=pltpu.HBM)
    return pl.pallas_call(
        body,
        out_shape=[VMEM(a.shape, a.dtype) for a in args],
        in_specs=[hbm] * len(args),
        out_specs=[pl.BlockSpec(memory_space=VMEM)] * len(args),
        scratch_shapes=[pltpu.SemaphoreType.DMA((len(args),))],
        compiler_params=pltpu.CompilerParams(vmem_limit_bytes=1 << 20),
        name="bring",
    )(*[pltpu.with_memory_space_constraint(a, pltpu.HBM) for a in args])


def sort_fields(orders, held):
    harmonics = orders.shape[1]
    blocks = harmonics // LANES
    arrays, (spots,) = listed(held)

    def body(orders_ref, *refs):
        out_ref, whole = refs[-2:]
        fill(whole, {slot: read(refs, e) for slot, e in spots.items()})
        targets = orders_ref[...] ^ (LANES - 1)
        chunk = 4 * LANES

        def step(c, carry):
            picked = jnp.dot(
                one_hot(targets, c * chunk, chunk), whole[...], preferred_element_type=F32
            ).astype(BF16)
            for b in range(chunk // LANES):
                re = picked[b * LANES : (b + 1) * LANES, :LANES]
                im = picked[b * LANES : (b + 1) * LANES, LANES:]
                at = pl.multiple_of((c * (chunk // LANES) + b) * 2 * LANES, LANES)
                out_ref[:LANES, pl.ds(at, LANES)] = re
                out_ref[:LANES, pl.ds(at + LANES, LANES)] = -im
                out_ref[LANES:, pl.ds(at, LANES)] = im
                out_ref[LANES:, pl.ds(at + LANES, LANES)] = re
            return carry

        lax.fori_loop(0, harmonics // chunk, step, 0)

    return call(
        body,
        VMEM((2 * LANES, blocks * 2 * LANES), BF16),
        [orders, *arrays],
        24,
        [VMEM((harmonics, 2 * LANES), BF16)],
    )


def chosen_pieces(refs, maps, slots):
    layer = lax.axis_index("layer")
    last = {slot: read(refs, maps[0][slot]) for slot in slots}
    own = dict(last)
    for index in range(1, len(maps)):
        for slot in slots:
            own[slot] = jnp.where(layer == index, read(refs, maps[index][slot]), own[slot])
    return last, own


def sort_chunks(orders_ref, whole, pieces, rows, band):
    harmonics = orders_ref.shape[1]
    first = harmonics - 1 - band * lax.axis_index("harm")
    held = []
    spot = 0
    for slot, value in pieces.items():
        size = value.shape[1]
        whole[spot : spot + size, :LANES] = value[0]
        whole[spot : spot + size, LANES:] = value[1]
        held.append(orders_ref[:, pl.ds(place(slot, size), size)])
        spot += size
    targets = jnp.concatenate(held, axis=1) + first
    chunk = 5 * LANES if rows % (5 * LANES) == 0 else LANES
    for row in range(0, rows, chunk):
        picked = jnp.dot(
            one_hot(targets, row, chunk), whole[...], preferred_element_type=F32
        ).astype(BF16)
        for b in range(chunk // LANES):
            yield row // LANES + b, picked[b * LANES : (b + 1) * LANES]


def begin(matrix, orders, sets, slots, band):
    rows = matrix.shape[1]
    harmonics = orders.shape[1]
    width = 2 * LANES
    window = harmonics + pl.cdiv(band, LANES) * LANES
    sets = [{slot: group[slot] for slot in slots} for group in sets]
    arrays, maps = listed(*sets)

    def body(matrix_ref, orders_ref, *refs):
        sums_ref, moved_ref, whole = refs[len(arrays) :]
        last, own = chosen_pieces(refs, maps, slots)
        by_re, by_im = partial_product(matrix_ref, last, zeros(matrix_ref))
        sums_ref[0] = by_re
        sums_ref[1] = by_im
        for block, picked in sort_chunks(orders_ref, whole, own, window, band):
            moved_ref[:, block * width : (block + 1) * width] = picked

    return call(
        body,
        [VMEM((2, rows, width), F32), VMEM((LANES, window // LANES * width), BF16)],
        [matrix, orders, *arrays],
        16,
        [VMEM((harmonics // len(ORDER) * len(slots), width), BF16)],
    )


def finish(matrix, orders, factors, sets, slots, begun, belows, band, scale):
    layers = len(sets)
    harmonics = orders.shape[1]
    rows = matrix.shape[1]
    blocks = harmonics // LANES
    strip = pl.cdiv(band, LANES) + 1
    width = 2 * LANES
    sets = [{slot: group[slot] for slot in slots} for group in sets]
    arrays, maps = listed(*sets)
    window = harmonics + (strip - 1) * LANES
    held = harmonics if slots == [WHOLE] else harmonics // len(ORDER) * len(slots)

    def body(matrix_ref, orders_ref, factors_ref, *refs):
        set_refs, refs = refs[: len(arrays)], refs[len(arrays) :]
        below_refs, refs = refs[: layers - 1], refs[layers - 1 :]
        begun_refs, refs = refs[: len(begun)], refs[len(begun) :]
        grad_ref, bottom_ref, whole, moved = refs
        layer = lax.axis_index("layer")
        last, own = chosen_pieces(set_refs, maps, slots)
        sums = (begun_refs[0][0], begun_refs[0][1]) if begun else zeros(matrix_ref)
        re, im = complex_product(partial_product(matrix_ref, last, sums))
        for index in range(1, layers):
            re = jnp.where(layer == index, below_refs[index - 1][0], re)
            im = jnp.where(layer == index, below_refs[index - 1][1], im)
        bottom_ref[0, 0] = re
        bottom_ref[0, 1] = im

        for block, picked in sort_chunks(orders_ref, whole, own, window, band):
            here = slice(block * width, (block + 1) * width)
            if begun:
                picked += begun_refs[1][:, here]
            moved[:LANES, here] = picked
            if block > 0:
                moved[LANES:, (block - 1) * width : block * width] = picked
        length = blocks * width
        parts = []
        for q in range(0, strip, 2):
            height = width if q + 1 < strip else LANES
            parts.append(
                lax.dot_general(
                    factors_ref[...],
                    moved[:height, q * width : q * width + length],
                    (((1,), (1,)), ((), ())),
                    preferred_element_type=F32,
                )
            )
        strips = jnp.concatenate(parts, axis=1)
        size = strip * LANES
        for part in range(2):
            skewed = pltpu.roll(
                strips[part * LANES : (part + 1) * LANES],
                size - (LANES - 1),
                1,
                stride=1,
                stride_axis=0,
            )
            total = jnp.sum(skewed[:, :band], axis=0, keepdims=True) * scale
            grad_ref[0, pl.ds(part, 1), :] = total

    outs = (
        jax.ShapeDtypeStruct((1, 2, band), F32),
        jax.ShapeDtypeStruct((1, 2, rows, LANES), BF16),
    )
    return call(
        body,
        outs,
        [matrix, orders, factors, *arrays, *belows, *begun],
        24,
        [
            VMEM((held, width), BF16),
            VMEM((2 * LANES, (blocks + strip - 1) * width), BF16),
        ],
    )


def sweep(*args):
    layers, count = lax.axis_size("layer"), lax.axis_size("harm")
    if layers > 2 and count == len(ORDER) and args[0].shape[1] % LANES == 0:
        return direct_sweep(*args)
    return gather_sweep(*args)


def sizes(source, orders):
    harmonics = orders.shape[0]
    band = 2 * harmonics // lax.axis_size("harm")
    return band, 1.0 / math.sqrt(harmonics * source.shape[2])


def gather_sweep(source, transfer, fields, orders):
    layers, count = lax.axis_size("layer"), lax.axis_size("harm")
    band, scale = sizes(source, orders)

    def gathered(value):
        return {WHOLE: (lax.all_gather(value, "harm", axis=1, tiled=True), None)}

    matrix, _, table = bring(transfer[0], source, orders.reshape(1, -1))
    group = gathered(source)
    sets, belows = [group], []
    for layer in range(layers - 1, 0, -1):
        below = propagate(matrix, group)
        pairs = [(layer * count + h, (layer - 1) * count + h) for h in range(count)]
        group = gathered(lax.ppermute(below, ("layer", "harm"), pairs))
        sets.append(group)
        belows.append(below)
    factors = sort_fields(table, gathered(fields[0]))
    return finish(
        matrix, table, factors, sets[::-1], [WHOLE], [], belows[::-1], band, scale
    )


def direct_sweep(source, transfer, fields, orders):
    layers, count = lax.axis_size("layer"), lax.axis_size("harm")
    band, scale = sizes(source, orders)
    top = layers - 1
    split = layers // 2

    def move(value, origin, target, slot):
        pairs = [(origin * count + h, target * count + t) for h, t in enumerate(route(slot))]
        return lax.ppermute(value, ("layer", "harm"), pairs)

    def among(value, members, slot):
        pairs = [
            (r * count + h, r * count + t) for r in members for h, t in enumerate(route(slot))
        ]
        return lax.ppermute(value, ("layer", "harm"), pairs)

    matrix, own, table = bring(transfer[0], source, orders.reshape(1, -1))
    group = {"own0": (own, None)}
    for slot in ORDER[:-1]:
        origin = top - 1 if slot[-1] == "1" and slot != "own1" else len(group) % split
        group[slot] = (move(source, origin, top, slot), None)
    along = [among(fields[0], range(layers), turn + "0") for turn in TURNS]

    sets, belows = [group], []
    for layer in range(top, 0, -1):
        below = propagate(matrix, group)
        group = {}
        for slot in ORDER:
            group[slot] = (move(below, layer, layer - 1, slot), None)
        sets.append(group)
        belows.append(below)
        if layer == top - 1:
            along, _ = lax.optimization_barrier((along, below))
            mine = jnp.stack([*along, fields[0]])
            beside = among(mine, range(layers), "own1")
    held = {}
    for part, turn in enumerate((*TURNS, "own")):
        held[turn + "0"] = (mine, part)
        held[turn + "1"] = (beside, part)
    factors = sort_fields(table, held)
    begun = begin(matrix, table, sets[::-1], EARLY, band)
    return finish(
        matrix, table, factors, sets[::-1], LATE, begun, belows[::-1], band, scale
    )


def solution(mesh):
    step = jax.shard_map(
        sweep,
        mesh=mesh,
        in_specs=(
            P(None, "harm", None),
            P("layer", None, "harm", None),
            P("layer", None, "harm", None),
            P(),
        ),
        out_specs=(P("layer", None, "harm"), P("layer", None, "harm", None)),
        check_vma=False,
    )
    if mesh.shape["harm"] != len(ORDER):
        return step
    return step
```

```python
import math

import jax
import jax.numpy as jnp
from jax import lax
from jax.experimental import pallas as pl
from jax.experimental.pallas import tpu as pltpu
from jax.sharding import PartitionSpec as P


LANES = 128
VMEM = pltpu.VMEM
BF16 = jnp.bfloat16
F32 = jnp.float32

QUARTERS = {
    "far": (3, 2, 1, 0),
    "out": (1, 3, 0, 2),
    "in": (2, 0, 3, 1),
    "near": (1, 0, 3, 2),
    "skip": (2, 3, 0, 1),
    "own": (0, 1, 2, 3),
}
ORDER = ("far0", "own1", "far1", "out0", "out1", "in0", "in1", "own0")
EARLY, LATE = list(ORDER[:4]), list(ORDER[4:])
SENT = [slot for slot in ORDER if slot != "own0"]
QUAD = ("near", "far", "own", "skip")
WHOLE = "all"


def route(slot):
    turn, swap = QUARTERS[slot[:-1]], int(slot[-1])
    half = len(ORDER) // len(turn)
    return [turn[h // half] * half + (h % half ^ swap) for h in range(len(ORDER))]


def place(slot, size):
    if slot == WHOLE:
        return 0
    targets = route(slot)
    here = lax.axis_index("harm")
    start = jnp.int32(targets.index(0) * size)
    for spot in range(1, len(targets)):
        start = jnp.where(here == spot, targets.index(spot) * size, start)
    return pl.multiple_of(start, size)


def listed(*sets):
    arrays, maps = [], []
    for group in sets:
        found = {}
        for slot, (value, part) in group.items():
            spot = next((i for i, a in enumerate(arrays) if a is value), len(arrays))
            if spot == len(arrays):
                arrays.append(value)
            found[slot] = (spot, part)
        maps.append(found)
    return arrays, maps


def read(refs, entry):
    spot, part = entry
    return refs[spot][...] if part is None else refs[spot][part]


def call(body, outs, args, limit, scratch=()):
    spec = pl.BlockSpec(memory_space=VMEM)
    return pl.pallas_call(
        body,
        out_shape=outs,
        in_specs=[spec] * len(args),
        out_specs=jax.tree.map(lambda _: spec, outs),
        scratch_shapes=list(scratch),
        compiler_params=pltpu.CompilerParams(vmem_limit_bytes=limit << 20),
    )(*[pltpu.with_memory_space_constraint(a, VMEM) for a in args])


def partial_product(matrix_ref, pieces, sums):
    by_re, by_im = sums
    for slot, value in pieces.items():
        size = value.shape[1]
        cols = pl.ds(place(slot, size), size)
        both = jnp.concatenate([value[0], value[1]], axis=1)
        by_re += jnp.dot(matrix_ref[0, :, cols], both, preferred_element_type=F32)
        by_im += jnp.dot(matrix_ref[1, :, cols], both, preferred_element_type=F32)
    return by_re, by_im


def zeros(matrix_ref):
    part = jnp.zeros((matrix_ref.shape[1], 2 * LANES), F32)
    return part, part


def complex_product(sums):
    by_re, by_im = sums
    re = by_re[:, :LANES] - by_im[:, LANES:]
    im = by_re[:, LANES:] + by_im[:, :LANES]
    return re.astype(BF16), im.astype(BF16)


def propagate(matrix, group):
    arrays, (spots,) = listed(group)

    def body(matrix_ref, *refs):
        out_ref = refs[-1]
        pieces = {slot: read(refs, e) for slot, e in spots.items()}
        re, im = complex_product(partial_product(matrix_ref, pieces, zeros(matrix_ref)))
        out_ref[0] = re
        out_ref[1] = im

    rows = matrix.shape[1]
    return call(body, VMEM((2, rows, LANES), BF16), [matrix, *arrays], 8)


def one_hot(targets, first, count):
    index = lax.broadcasted_iota(jnp.int32, (count, targets.shape[1]), 0) + first
    return jnp.where(index == targets, 1.0, 0.0).astype(BF16)


def fill(whole, pieces):
    for slot, value in pieces.items():
        rows = pl.ds(place(slot, value.shape[1]), value.shape[1])
        whole[rows, :LANES] = value[0]
        whole[rows, LANES:] = value[1]


def bring(*args):
    def body(*refs):
        size = len(args)
        ins, outs, sems = refs[:size], refs[size : 2 * size], refs[-1]
        copies = [
            pltpu.make_async_copy(ins[i], outs[i], sems.at[i]) for i in range(size)
        ]
        for copy in copies:
            copy.start()
        for copy in copies:
            copy.wait()

    hbm = pl.BlockSpec(memory_space=pltpu.HBM)
    return pl.pallas_call(
        body,
        out_shape=[VMEM(a.shape, a.dtype) for a in args],
        in_specs=[hbm] * len(args),
        out_specs=[pl.BlockSpec(memory_space=VMEM)] * len(args),
        scratch_shapes=[pltpu.SemaphoreType.DMA((len(args),))],
        compiler_params=pltpu.CompilerParams(vmem_limit_bytes=1 << 20),
        name="bring",
    )(*[pltpu.with_memory_space_constraint(a, pltpu.HBM) for a in args])


def sort_fields(orders, held):
    harmonics = orders.shape[1]
    blocks = harmonics // LANES
    arrays, (spots,) = listed(held)

    def body(orders_ref, *refs):
        out_ref, whole = refs[-2:]
        fill(whole, {slot: read(refs, e) for slot, e in spots.items()})
        targets = orders_ref[...] ^ (LANES - 1)
        chunk = 4 * LANES

        def step(c, carry):
            picked = jnp.dot(
                one_hot(targets, c * chunk, chunk), whole[...], preferred_element_type=F32
            ).astype(BF16)
            for b in range(chunk // LANES):
                re = picked[b * LANES : (b + 1) * LANES, :LANES]
                im = picked[b * LANES : (b + 1) * LANES, LANES:]
                at = pl.multiple_of((c * (chunk // LANES) + b) * 2 * LANES, LANES)
                out_ref[:LANES, pl.ds(at, LANES)] = re
                out_ref[:LANES, pl.ds(at + LANES, LANES)] = -im
                out_ref[LANES:, pl.ds(at, LANES)] = im
                out_ref[LANES:, pl.ds(at + LANES, LANES)] = re
            return carry

        lax.fori_loop(0, harmonics // chunk, step, 0)

    return call(
        body,
        VMEM((2 * LANES, blocks * 2 * LANES), BF16),
        [orders, *arrays],
        24,
        [VMEM((harmonics, 2 * LANES), BF16)],
    )


def chosen_pieces(refs, maps, slots):
    layer = lax.axis_index("layer")
    last = {slot: read(refs, maps[0][slot]) for slot in slots}
    own = dict(last)
    for index in range(1, len(maps)):
        for slot in slots:
            own[slot] = jnp.where(layer == index, read(refs, maps[index][slot]), own[slot])
    return last, own


def sort_chunks(orders_ref, whole, pieces, rows, band):
    harmonics = orders_ref.shape[1]
    first = harmonics - 1 - band * lax.axis_index("harm")
    held = []
    spot = 0
    for slot, value in pieces.items():
        size = value.shape[1]
        whole[spot : spot + size, :LANES] = value[0]
        whole[spot : spot + size, LANES:] = value[1]
        held.append(orders_ref[:, pl.ds(place(slot, size), size)])
        spot += size
    targets = jnp.concatenate(held, axis=1) + first
    chunk = 5 * LANES if rows % (5 * LANES) == 0 else LANES
    for row in range(0, rows, chunk):
        picked = jnp.dot(
            one_hot(targets, row, chunk), whole[...], preferred_element_type=F32
        ).astype(BF16)
        for b in range(chunk // LANES):
            yield row // LANES + b, picked[b * LANES : (b + 1) * LANES]


def begin(matrix, orders, sets, slots, band):
    rows = matrix.shape[1]
    harmonics = orders.shape[1]
    width = 2 * LANES
    window = harmonics + pl.cdiv(band, LANES) * LANES
    sets = [{slot: group[slot] for slot in slots} for group in sets]
    arrays, maps = listed(*sets)

    def body(matrix_ref, orders_ref, *refs):
        sums_ref, moved_ref, whole = refs[len(arrays) :]
        last, own = chosen_pieces(refs, maps, slots)
        by_re, by_im = partial_product(matrix_ref, last, zeros(matrix_ref))
        sums_ref[0] = by_re
        sums_ref[1] = by_im
        for block, picked in sort_chunks(orders_ref, whole, own, window, band):
            moved_ref[:, block * width : (block + 1) * width] = picked

    return call(
        body,
        [VMEM((2, rows, width), F32), VMEM((LANES, window // LANES * width), BF16)],
        [matrix, orders, *arrays],
        16,
        [VMEM((harmonics // len(ORDER) * len(slots), width), BF16)],
    )


def finish(matrix, orders, factors, sets, slots, begun, belows, band, scale):
    layers = len(sets)
    harmonics = orders.shape[1]
    rows = matrix.shape[1]
    blocks = harmonics // LANES
    strip = pl.cdiv(band, LANES) + 1
    width = 2 * LANES
    sets = [{slot: group[slot] for slot in slots} for group in sets]
    arrays, maps = listed(*sets)
    window = harmonics + (strip - 1) * LANES
    held = harmonics if slots == [WHOLE] else harmonics // len(ORDER) * len(slots)

    def body(matrix_ref, orders_ref, factors_ref, *refs):
        set_refs, refs = refs[: len(arrays)], refs[len(arrays) :]
        below_refs, refs = refs[: layers - 1], refs[layers - 1 :]
        begun_refs, refs = refs[: len(begun)], refs[len(begun) :]
        grad_ref, bottom_ref, whole, moved = refs
        layer = lax.axis_index("layer")
        last, own = chosen_pieces(set_refs, maps, slots)
        sums = (begun_refs[0][0], begun_refs[0][1]) if begun else zeros(matrix_ref)
        re, im = complex_product(partial_product(matrix_ref, last, sums))
        for index in range(1, layers):
            re = jnp.where(layer == index, below_refs[index - 1][0], re)
            im = jnp.where(layer == index, below_refs[index - 1][1], im)
        bottom_ref[0, 0] = re
        bottom_ref[0, 1] = im

        for block, picked in sort_chunks(orders_ref, whole, own, window, band):
            here = slice(block * width, (block + 1) * width)
            if begun:
                picked += begun_refs[1][:, here]
            moved[:LANES, here] = picked
            if block > 0:
                moved[LANES:, (block - 1) * width : block * width] = picked
        length = blocks * width
        parts = []
        for q in range(0, strip, 2):
            height = width if q + 1 < strip else LANES
            parts.append(
                lax.dot_general(
                    factors_ref[...],
                    moved[:height, q * width : q * width + length],
                    (((1,), (1,)), ((), ())),
                    preferred_element_type=F32,
                )
            )
        strips = jnp.concatenate(parts, axis=1)
        size = strip * LANES
        for part in range(2):
            skewed = pltpu.roll(
                strips[part * LANES : (part + 1) * LANES],
                size - (LANES - 1),
                1,
                stride=1,
                stride_axis=0,
            )
            total = jnp.sum(skewed[:, :band], axis=0, keepdims=True) * scale
            grad_ref[0, pl.ds(part, 1), :] = total

    outs = (
        jax.ShapeDtypeStruct((1, 2, band), F32),
        jax.ShapeDtypeStruct((1, 2, rows, LANES), BF16),
    )
    return call(
        body,
        outs,
        [matrix, orders, factors, *arrays, *belows, *begun],
        24,
        [
            VMEM((held, width), BF16),
            VMEM((2 * LANES, (blocks + strip - 1) * width), BF16),
        ],
    )


def sweep(*args):
    layers, count = lax.axis_size("layer"), lax.axis_size("harm")
    if layers > 2 and count == len(ORDER) and args[0].shape[1] % LANES == 0:
        return direct_sweep(*args)
    return gather_sweep(*args)


def sizes(source, orders):
    harmonics = orders.shape[0]
    band = 2 * harmonics // lax.axis_size("harm")
    return band, 1.0 / math.sqrt(harmonics * source.shape[2])


def gather_sweep(source, transfer, fields, orders):
    layers, count = lax.axis_size("layer"), lax.axis_size("harm")
    band, scale = sizes(source, orders)

    def gathered(value):
        return {WHOLE: (lax.all_gather(value, "harm", axis=1, tiled=True), None)}

    matrix, table = bring(transfer[0], orders.reshape(1, -1))
    group = gathered(source)
    sets, belows = [group], []
    for layer in range(layers - 1, 0, -1):
        below = propagate(matrix, group)
        pairs = [(layer * count + h, (layer - 1) * count + h) for h in range(count)]
        group = gathered(lax.ppermute(below, ("layer", "harm"), pairs))
        sets.append(group)
        belows.append(below)
    factors = sort_fields(table, gathered(fields[0]))
    return finish(
        matrix, table, factors, sets[::-1], [WHOLE], [], belows[::-1], band, scale
    )


def direct_sweep(source, transfer, fields, orders):
    layers, count = lax.axis_size("layer"), lax.axis_size("harm")
    band, scale = sizes(source, orders)
    top = layers - 1
    split = layers // 2

    def move(value, origin, target, slot):
        pairs = [(origin * count + h, target * count + t) for h, t in enumerate(route(slot))]
        return lax.ppermute(value, ("layer", "harm"), pairs)

    def among(value, members, slot):
        pairs = [
            (r * count + h, r * count + t) for r in members for h, t in enumerate(route(slot))
        ]
        return lax.ppermute(value, ("layer", "harm"), pairs)

    matrix, own = bring(transfer[0], source)
    (table,) = bring(orders.reshape(1, -1))
    group = {"own0": (own, None)}
    for slot in SENT:
        origin = top - 1 if slot[-1] == "1" and slot != "own1" else len(group) % split
        group[slot] = (move(source, origin, top, slot), None)
    skipped = among(fields[0], range(layers), "skip0")

    sets, belows = [group], []
    for layer in range(top, 0, -1):
        below = propagate(matrix, group)
        group = {}
        for slot in ORDER:
            group[slot] = (move(below, layer, layer - 1, slot), None)
        sets.append(group)
        belows.append(below)
        if layer == top:
            skipped, _ = lax.optimization_barrier((skipped, below))
            pair = jnp.stack([fields[0], skipped])
            near = among(pair, range(layers), "near0")
        if layer == top - 1:
            near, _ = lax.optimization_barrier((near, below))
            mine = jnp.concatenate([near, pair])
            beside = among(mine, range(layers), "own1")
    held = {}
    for part, turn in enumerate(QUAD):
        held[turn + "0"] = (mine, part)
        held[turn + "1"] = (beside, part)
    factors = sort_fields(table, held)
    begun = begin(matrix, table, sets[::-1], EARLY, band)
    return finish(
        matrix, table, factors, sets[::-1], LATE, begun, belows[::-1], band, scale
    )


def solution(mesh):
    step = jax.shard_map(
        sweep,
        mesh=mesh,
        in_specs=(
            P(None, "harm", None),
            P("layer", None, "harm", None),
            P("layer", None, "harm", None),
            P(),
        ),
        out_specs=(P("layer", None, "harm"), P("layer", None, "harm", None)),
        check_vma=False,
    )
    if mesh.shape["harm"] != len(ORDER):
        return step
    return step
```
